256 devices in a mesh: gx: 16 (over z_lo, x), gy: 4 (over y), gz: 4 (over z_hi, core).
Axes of the slice: x: 4, y: 4, z: 8 (z_hi: 2, z_lo: 4; z = z_hi * 4 + z_lo), core: 2. Of those that a mesh axis runs over, the one named last changes fastest.
Arguments:
- displacement: float32 [3, 128, 32, 512], P(None, 'gx', 'gz', 'gy'), may hold values from -0.1 to 0.1
- velocity: float32 [3, 128, 32, 512], P(None, 'gx', 'gz', 'gy'), may hold values from -0.4 to 0.4
- body_force: float32 [3, 128, 32, 512], P(None, 'gx', 'gz', 'gy'), may hold values from -4 to 4
- broken: int32 [12, 128, 32, 512], P(None, 'gx', 'gz', 'gy'), may hold values from 0 to 1073741823
Outputs:
- new_displacement: float32 [3, 128, 32, 512], P(None, 'gx', 'gz', 'gy')
- new_velocity: float32 [3, 128, 32, 512], P(None, 'gx', 'gz', 'gy')
- new_acceleration: float32 [3, 128, 32, 512], P(None, 'gx', 'gz', 'gy')
- strain_energy: float32 [], replicated
The draws below stay inside these ranges and needn't reach their ends.
All inputs are finite; a program needn't handle non-finite values.
Results may differ from the reference program's by a relative error of at most 0.0003.
Values sent between devices are 32-bit elements; how exact they have to be, the bound alone decides.
A program may use at most 128 MiB of HBM per device.

```python
import math
import jax
import jax.numpy as jnp
from jax import lax

CX = 8
WORDS = 12
NX = 128
NZ = 32
NY = 512


def draw_displacement(key, part):
    key_noise = jax.random.fold_in(key, 11)
    along_x = (jnp.arange(NX, dtype=jnp.float32) + 0.5) / NX
    noise = jax.random.normal(key_noise, (3, NX, NZ, NY), jnp.float32)
    values = noise * (0.03 * (0.5 + along_x))[None, :, None, None]
    return jnp.clip(values, -0.1, 0.1)


def place_ends(result, own_key, low, high):
    longest = result.shape.index(max(result.shape))
    spots = []
    for shift in (0, 1):
        where = [jax.random.randint(jax.random.fold_in(own_key, axis), (), 0, length) for axis, length in enumerate(result.shape)]
        where[longest] = (where[longest] + shift) % result.shape[longest]
        spots.append(tuple(where))
    return result.at[spots[0]].set(low).at[spots[1]].set(high)


def block_levels(own_key, dims, split, least, high):
    factor_of, own = 1.0, jax.random.fold_in(own_key, 6)
    for axis_at, blocks in split:
        heights = jnp.exp(jax.random.uniform(jax.random.fold_in(own, axis_at), (blocks,), jnp.float32, least / len(split), high / len(split)))
        factor_of = factor_of * jnp.repeat(heights, dims[axis_at] // blocks).reshape([-1 if axis == axis_at else 1 for axis in range(len(dims))])
    return factor_of


def bell_draw(own_key, shape, width, most, split=(), held_as=jnp.bfloat16):
    entries = jax.random.normal(own_key, shape, jnp.float32) * width
    if len(split) > 0:
        entries = block_levels(own_key, shape, split, -0.22, 0.18) * entries
    return jnp.clip(entries, min=-most, max=most).astype(held_as)


def setup_inputs(seed: int = 0) -> dict:
    seeds = jax.random.split(jax.random.key(seed), 5)
    displacement = draw_displacement(jax.random.fold_in(seeds[4], 71), 0)
    velocity = bell_draw(seeds[1], (3, NX, NZ, NY), 0.15, 0.4, ((1, 16), (2, 4), (3, 4)), jnp.float32)
    body_force = bell_draw(seeds[2], (3, NX, NZ, NY), 1.0, 4.0, ((1, 16), (2, 4), (3, 4)), jnp.float32)
    broken = place_ends(jax.random.randint(seeds[3], (WORDS, NX, NZ, NY), 0, 1073741824), jax.random.fold_in(seeds[3], 1), 0, 1073741823).astype(jnp.int32)
    return dict(displacement=displacement, velocity=velocity, body_force=body_force, broken=broken)


TIME_STEP = 0.05
MICRO_MODULUS = 4.0
BITS_PER_WORD = 30
OFFSET_LIST = tuple(((step_x, step_z, step_y) for step_x in range(-3, 4) for step_z in range(-3, 4) for step_y in range(-3, 4) if (step_x, step_z, step_y) != (0, 0, 0)))

def bond_sum(extended, mask_block, depth_start, depth_total, row_count, depth_count, width_count, with_energy):
    center = extended[:, 3:3 + row_count, 3:3 + depth_count, 3:3 + width_count]
    depth_index = depth_start + jnp.arange(depth_count, dtype=jnp.int32)
    force_x = jnp.zeros(center.shape[1:], jnp.float32)
    force_z = jnp.zeros(center.shape[1:], jnp.float32)
    force_y = jnp.zeros(center.shape[1:], jnp.float32)
    energy = jnp.zeros(center.shape[1:], jnp.float32)
    for bond_index, (step_x, step_z, step_y) in enumerate(OFFSET_LIST):
        neighbour = extended[:, 3 + step_x:3 + step_x + row_count, 3 + step_z:3 + step_z + depth_count, 3 + step_y:3 + step_y + width_count]
        relative = neighbour - center
        bond_x = relative[0] + step_x
        bond_z = relative[1] + step_z
        bond_y = relative[2] + step_y
        length = jnp.sqrt(bond_x * bond_x + bond_z * bond_z + bond_y * bond_y)
        rest_length = math.sqrt(step_x * step_x + step_z * step_z + step_y * step_y)
        influence = math.exp(-rest_length * rest_length / 9.0)
        stretch = (length - rest_length) / rest_length
        broken_bit = jnp.right_shift(mask_block[bond_index // BITS_PER_WORD], bond_index % BITS_PER_WORD) & 1
        inside = (depth_index + step_z >= 0) & (depth_index + step_z < depth_total)
        intact = jnp.where(inside[None, :, None], 1 - broken_bit, 0).astype(jnp.float32)
        factor = intact * (MICRO_MODULUS * influence) * stretch / length
        force_x = force_x + factor * bond_x
        force_z = force_z + factor * bond_z
        force_y = force_y + factor * bond_y
        if with_energy:
            energy = energy + intact * (0.25 * MICRO_MODULUS * influence * rest_length) * stretch * stretch
    return (jnp.stack([force_x, force_z, force_y]), jnp.sum(energy))

def slab_forces(field_in, broken, with_energy):
    padded = jnp.pad(field_in, ((0, 0), (3, 3), (3, 3), (3, 3)), mode='wrap')
    starts = jnp.arange(NX // CX, dtype=jnp.int32) * CX

    def block_force(first_row):
        first_row = first_row.astype(jnp.int32)
        anchor = jnp.zeros((), jnp.int32)
        extended = lax.dynamic_slice(padded, (anchor, first_row, anchor, anchor), (3, CX + 6, NZ + 6, NY + 6))
        mask_block = lax.dynamic_slice(broken, (anchor, first_row, anchor, anchor), (WORDS, CX, NZ, NY))
        return bond_sum(extended, mask_block, 0, NZ, CX, NZ, NY, with_energy)
    pieces, energies = lax.map(block_force, starts)
    forces = jnp.moveaxis(pieces, 0, 1).reshape(3, NX, NZ, NY)
    return (forces, jnp.sum(energies))

def reference(displacement, velocity, body_force, broken):
    first_force, unused = slab_forces(displacement, broken, False)
    first_acceleration = first_force + body_force
    new_displacement = displacement + TIME_STEP * velocity + 0.5 * TIME_STEP * TIME_STEP * first_acceleration
    second_force, energy = slab_forces(new_displacement, broken, True)
    new_acceleration = second_force + body_force
    new_velocity = velocity + 0.5 * TIME_STEP * (first_acceleration + new_acceleration)
    strain_energy = energy / jnp.float32(NX * NY)
    return (new_displacement, new_velocity, new_acceleration, strain_energy)
```

```python
import functools
import math

import jax
import jax.numpy as jnp
from jax import lax
from jax.experimental import pallas as pl
from jax.experimental.pallas import tpu as pltpu
from jax.sharding import PartitionSpec as P

MESH = pl.DeviceIdType.MESH
TIME_STEP = 0.05
BITS_PER_WORD = 30
SIDE_X = 4
R = 3
NB = 8
EXT = NB + 2 * R
LANES = 128
REACH = range(-R, R + 1)

FAR = [
    (ez, ex, ey) for ez in (-1, 1) for ex in (0, -1, 1) for ey in (0, -1, 1)
]
NEAR = [(0, ex, ey) for ex in (0, -1, 1) for ey in (0, -1, 1) if (ex, ey) != (0, 0)]
SOURCES = FAR + NEAR
SLOT = {e: i for i, e in enumerate(SOURCES)}

CLASSES = {}
for _p in REACH:
    for _r in REACH:
        CLASSES.setdefault(_p * _p + _r * _r, []).append((_p, _r))
CLASSES = sorted(CLASSES.items())


def side(e):
    return 0 if e < 0 else 1


def bond_number(p, q, r):
    flat = (p + R) * 49 + (q + R) * 7 + (r + R)
    return flat if flat < 171 else flat - 1


def weight(p, q, r):
    return 4.0 * math.exp(-(p * p + q * q + r * r) / 9.0)


def kernel(
    sizes,
    disp,
    vel,
    body,
    broken,
    newd_out,
    newv_out,
    newa_out,
    energy_out,
    core,
    xpack,
    ypack,
    zrecv,
    xrecv,
    zxrecv,
    yrecv,
    yext,
    ext,
    bonds,
    force,
    esum,
    erow,
    eplane,
    ecol,
    send_sem,
    recv_sem,
    esend_sem,
    erecv_sem,
):
    n_gx, n_gy, n_gz = sizes
    gx, gy, gz = lax.axis_index("gx"), lax.axis_index("gy"), lax.axis_index("gz")
    has_low, has_high = gz > 0, gz < n_gz - 1

    def at(ez, ex, ey):
        return (
            lax.rem(gx + ex + n_gx, n_gx),
            lax.rem(gy + ey + n_gy, n_gy),
            gz + ez,
        )

    side_x = SIDE_X
    n_plane = side_x * n_gy * 2
    n_col = (n_gx // side_x) * (n_gz // 2)
    my_x, my_zlo = lax.rem(gx, side_x), gx // side_x
    my_core, my_zhi = lax.rem(gz, 2), gz // 2
    my_plane = (my_x * n_gy + gy) * 2 + my_core
    my_col = my_zhi * (n_gx // side_x) + my_zlo

    def plane_device(m):
        return (
            my_zlo * side_x + m // (2 * n_gy),
            lax.rem(m // 2, n_gy),
            my_zhi * 2 + lax.rem(m, 2),
        )

    def col_device(m):
        return (
            lax.rem(m, n_gx // side_x) * side_x + my_x,
            gy,
            (m // (n_gx // side_x)) * 2 + my_core,
        )

    barrier = pltpu.get_barrier_semaphore()

    def greet(device):
        pl.semaphore_signal(barrier, inc=1, device_id=device, device_id_type=MESH)

    for present, low in ((has_low, True), (has_high, False)):

        @pl.when(present)
        def _(low=low):
            for e in FAR:
                if (e[0] < 0) == low:
                    greet(at(*e))

    for e in NEAR:
        greet(at(*e))

    @pl.loop(1, n_plane)
    def _(j):
        greet(plane_device(lax.rem(my_plane + j, n_plane)))

    @pl.loop(1, n_col)
    def _(j):
        greet(col_device(lax.rem(my_col + j, n_col)))

    lane = lax.broadcasted_iota(jnp.int32, (NB, LANES), 1)
    lane2 = lax.broadcasted_iota(jnp.int32, (2 * NB, LANES), 1)

    for present, low in ((has_low, True), (has_high, False)):

        @pl.when(jnp.logical_not(present))
        def _(low=low):
            s = 0 if low else 1
            for step in (0, 1):
                zrecv[step, s] = jnp.zeros(zrecv.shape[2:], jnp.float32)
                zxrecv[step, s] = jnp.zeros(zxrecv.shape[2:], jnp.float32)
                for e in FAR:
                    if (e[0] < 0) == low and e[2] != 0:
                        yrecv[step, SLOT[e]] = jnp.zeros((NB, LANES), jnp.float32)

    def message(step, e):
        ez, ex, ey = e
        slot = SLOT[e]
        if ey != 0:
            src, dst = ypack.at[step, side(ey)], yrecv.at[step, slot]
        elif ex == 0:
            src = core.at[step, pl.ds(NB - R if ez < 0 else 0, R)]
            dst = zrecv.at[step, side(ez)]
        elif ez == 0:
            src, dst = xpack.at[step, side(ex)], xrecv.at[step, side(ex)]
        else:
            src = xpack.at[step, side(ex), pl.ds(40 if ez < 0 else 0, 32)]
            dst = zxrecv.at[step, side(ez), side(ex)]
        return pltpu.make_async_remote_copy(
            src_ref=src,
            dst_ref=dst,
            send_sem=send_sem.at[step, slot],
            recv_sem=recv_sem.at[step, slot],
            device_id=at(-ez, -ex, -ey),
            device_id_type=MESH,
        )

    def send(step):
        for present, up in ((has_high, True), (has_low, False)):

            @pl.when(present)
            def _(up=up):
                for e in FAR:
                    if (e[0] < 0) == up:
                        message(step, e).start()

        for e in NEAR:
            message(step, e).start()

    def receive_far(step):
        for present, low in ((has_low, True), (has_high, False)):

            @pl.when(present)
            def _(low=low):
                for e in FAR:
                    if (e[0] < 0) == low:
                        message(step, e).wait_recv()

    def finish_sends(step):
        for present, up in ((has_high, True), (has_low, False)):

            @pl.when(present)
            def _(up=up):
                for e in FAR:
                    if (e[0] < 0) == up:
                        message(step, e).wait_send()

        for e in NEAR:
            message(step, e).wait_send()

    def pack(step):
        ylow = jnp.zeros((NB, LANES), jnp.float32)
        yhigh = jnp.zeros((NB, LANES), jnp.float32)
        for z in range(NB):
            for c in range(3):
                g = 3 * (z * 3 + c)
                value = core[step, z, c]
                ext[R, z + R, c, R : R + NB, :] = value
                xpack[step, 0, g : g + R, :] = core[step, z, c, NB - R : NB, :]
                xpack[step, 1, g : g + R, :] = core[step, z, c, 0:R, :]
                mine = (lane >= g) & (lane < g + R)
                ylow = jnp.where(mine, pltpu.roll(value, (g + R) % LANES, 1), ylow)
                yhigh = jnp.where(mine, pltpu.roll(value, g, 1) if g else value, yhigh)
        ypack[step, 0] = ylow
        ypack[step, 1] = yhigh

    def fill_rows(step, ez):
        first, count, base = (
            (0, R, NB - R) if ez < 0 else (R, NB, 0) if ez == 0 else (R + NB, R, 0)
        )
        lead = 40 if ez < 0 else 0
        for i in range(count):
            for c in range(3):
                g = 3 * ((base + i) * 3 + c) - lead
                if ez != 0:
                    ext[R, first + i, c, R : R + NB, :] = zrecv[step, side(ez), i, c]
                for s, row in ((0, 0), (1, R + NB)):
                    if ez == 0:
                        strip = xrecv[step, s, g : g + R, :]
                    else:
                        strip = zxrecv[step, side(ez), s, g : g + R, :]
                    ext[R, first + i, c, row : row + R, :] = strip
        for s, ey in ((0, -1), (1, 1)):
            yext[s, R : R + NB, :] = yrecv[step, SLOT[(ez, 0, ey)]]
            yext[s, 0:R, :] = yrecv[step, SLOT[(ez, -1, ey)], NB - R : NB, :]
            yext[s, R + NB : EXT, :] = yrecv[step, SLOT[(ez, 1, ey)], 0:R, :]

        @pl.loop(0, count)
        def _(i):
            for c in range(3):
                g = 3 * ((base + i) * 3 + c)
                left = pltpu.roll(yext[0], lax.rem(2 * LANES - R - g, LANES), 1)
                right = pltpu.roll(yext[1], lax.rem(LANES - g, LANES), 1)
                here = ext[R, first + i, c]
                for r in range(1, R + 1):
                    ext[R + r, first + i, c] = pltpu.roll(
                        jnp.where(lane2 < r, right, here), LANES - r, 1
                    )
                    ext[R - r, first + i, c] = pltpu.roll(
                        jnp.where(lane2 >= LANES - r, left, here), r, 1
                    )

    def unpack_bonds():
        @pl.loop(0, NB)
        def _(z):
            words = [broken[w, pl.ds(z, NB, stride=NB), :] for w in range(12)]
            depth = gz * NB + z
            for q in REACH:
                inside = (depth + q >= 0) & (depth + q < n_gz * NB)
                scale = jnp.where(inside, 1.0, 0.0)
                for _, members in CLASSES:
                    whole = jnp.full(
                        (NB, LANES), scale * weight(members[0][0], q, members[0][1])
                    )
                    for p, r in members:
                        j = (p + R) * 7 + r + R
                        if (p, q, r) == (0, 0, 0):
                            bonds[z, q + R, j] = jnp.zeros((NB, LANES), jnp.float32)
                            continue
                        k = bond_number(p, q, r)
                        bit = words[k // BITS_PER_WORD] & (1 << (k % BITS_PER_WORD))
                        bonds[z, q + R, j] = jnp.where(bit == 0, whole, 0.0)

    def add_row(step, z, q, with_energy):
        cx, cz, cy = (core[step, z, c] for c in range(3))
        cz = cz - q.astype(jnp.float32)
        cxs = {p: cx - float(p) if p else cx for p in REACH}
        cys = {r: cy - float(r) if r else cy for r in REACH}
        row = z + q + R
        fx = fz = fy = energy = None

        def plus(a, b):
            return b if a is None else a + b

        for square, members in CLASSES:
            own = jnp.where(q == 0, 1, 0) if square == 0 else 0
            rest_square = (q * q + square + own).astype(jnp.float32)
            inverse_rest = lax.rsqrt(jnp.full((NB, LANES), rest_square))
            class_energy = None
            for p, r in members:
                there = ext.at[r + R, row]
                bx = there[0, R + p : R + p + NB, :] - cxs[p]
                bz = there[1, R + p : R + p + NB, :] - cz
                by = there[2, R + p : R + p + NB, :] - cys[r]
                length_square = bx * bx + bz * bz + by * by
                if square == 0:
                    length_square = length_square + own.astype(jnp.float32)
                gap = inverse_rest - lax.rsqrt(length_square)
                pull = bonds[z, q + R, (p + R) * 7 + r + R] * gap
                fx = plus(fx, pull * bx)
                fz = plus(fz, pull * bz)
                fy = plus(fy, pull * by)
                if with_energy:
                    class_energy = plus(class_energy, pull * gap * length_square)
            if with_energy:
                rest = jnp.full((NB, LANES), rest_square) * inverse_rest
                energy = plus(energy, class_energy * rest)
        force[step, z, 0] += fx
        force[step, z, 1] += fz
        force[step, z, 2] += fy
        if with_energy:
            esum[...] += energy

    def add_pair(step, z, q, with_energy):
        add_row(step, z, q, with_energy)
        add_row(step, NB - 1 - z, -q, with_energy)

    def inner_rows(step, with_energy):
        @pl.loop(0, R + 1)
        def _(q):
            @pl.loop(0, jnp.where(q == 0, NB // 2, NB - q))
            def _(z):
                add_pair(step, z, q, with_energy)

    def outer_rows(step, with_energy):
        @pl.loop(1, R + 1)
        def _(q):
            @pl.loop(NB - q, NB)
            def _(z):
                add_pair(step, z, q, with_energy)

    def exchange_and_sum(step, with_energy, between):
        pack(step)
        if step == 0:
            greeted = (
                len(NEAR)
                + (len(FAR) // 2)
                * (jnp.where(has_low, 1, 0) + jnp.where(has_high, 1, 0))
                + n_plane
                - 1
                + n_col
                - 1
            )
            pl.semaphore_wait(barrier, greeted)
        send(step)
        between()
        for e in NEAR:
            message(step, e).wait_recv()
        fill_rows(step, 0)
        inner_rows(step, with_energy)
        receive_far(step)
        fill_rows(step, -1)
        fill_rows(step, 1)
        outer_rows(step, with_energy)

    def start_force(step):
        @pl.loop(0, NB)
        def _(z):
            for c in range(3):
                force[step, z, c] = body[c, pl.ds(z, NB, stride=NB), :]

    def before_first():
        unpack_bonds()
        start_force(0)

    @pl.loop(0, NB)
    def _(z):
        for c in range(3):
            core[0, z, c] = disp[c, pl.ds(z, NB, stride=NB), :]

    exchange_and_sum(0, False, before_first)

    @pl.loop(0, NB)
    def _(z):
        for c in range(3):
            rows = pl.ds(z, NB, stride=NB)
            moved = (
                core[0, z, c]
                + TIME_STEP * vel[c, rows, :]
                + (0.5 * TIME_STEP * TIME_STEP) * force[0, z, c]
            )
            core[1, z, c] = moved
            newd_out[c, rows, :] = moved

    esum[...] = jnp.zeros((NB, LANES), jnp.float32)
    exchange_and_sum(1, True, lambda: start_force(1))

    erow[0] = jnp.sum(esum[...], axis=0, keepdims=True)
    eplane[my_plane] = erow[0]

    def plane_message(j, slot, device):
        return pltpu.make_async_remote_copy(
            src_ref=erow.at[0],
            dst_ref=eplane.at[slot],
            send_sem=esend_sem.at[0, j],
            recv_sem=erecv_sem.at[0, j],
            device_id=plane_device(device),
            device_id_type=MESH,
        )

    @pl.loop(1, n_plane)
    def _(j):
        plane_message(j, my_plane, lax.rem(my_plane + j, n_plane)).start()

    @pl.loop(0, NB)
    def _(z):
        for c in range(3):
            rows = pl.ds(z, NB, stride=NB)
            newa = force[1, z, c]
            newa_out[c, rows, :] = newa
            newv_out[c, rows, :] = vel[c, rows, :] + (0.5 * TIME_STEP) * (
                force[0, z, c] + newa
            )

    finish_sends(0)
    finish_sends(1)

    @pl.loop(1, n_plane)
    def _(j):
        other = lax.rem(my_plane - j + n_plane, n_plane)
        plane_message(j, other, other).wait()

    total = eplane[0]
    for m in range(1, n_plane):
        total = total + eplane[m]
    erow[1] = total
    ecol[my_col] = total

    def col_message(j, slot, device):
        return pltpu.make_async_remote_copy(
            src_ref=erow.at[1],
            dst_ref=ecol.at[slot],
            send_sem=esend_sem.at[1, j],
            recv_sem=erecv_sem.at[1, j],
            device_id=col_device(device),
            device_id_type=MESH,
        )

    @pl.loop(1, n_col)
    def _(j):
        col_message(j, my_col, lax.rem(my_col + j, n_col)).start()

    @pl.loop(1, n_col)
    def _(j):
        other = lax.rem(my_col - j + n_col, n_col)
        col_message(j, other, other).wait()

    total = ecol[0]
    for m in range(1, n_col):
        total = total + ecol[m]
    area = (n_gx * NB) * (n_gy * LANES)
    energy_out[0, 0] = jnp.sum(total) * (0.25 / area)


def solution(mesh):
    sizes = (mesh.shape["gx"], mesh.shape["gy"], mesh.shape["gz"])
    f32 = jnp.float32
    block = jax.ShapeDtypeStruct((3, NB * NB, LANES), f32)

    def step(displacement, velocity, body_force, broken):
        flat = [
            a.reshape(a.shape[0], NB * NB, LANES)
            for a in (displacement, velocity, body_force, broken)
        ]
        newd, newv, newa, energy = pl.pallas_call(
            functools.partial(kernel, sizes),
            out_shape=(block, block, block, jax.ShapeDtypeStruct((1, 1), f32)),
            in_specs=[pl.BlockSpec(memory_space=pltpu.VMEM)] * 4,
            out_specs=[pl.BlockSpec(memory_space=pltpu.VMEM)] * 3
            + [pl.BlockSpec(memory_space=pltpu.SMEM)],
            scratch_shapes=[
                pltpu.VMEM((2, NB, 3, NB, LANES), f32),
                pltpu.VMEM((2, 2, 72, LANES), f32),
                pltpu.VMEM((2, 2, NB, LANES), f32),
                pltpu.VMEM((2, 2, R, 3, NB, LANES), f32),
                pltpu.VMEM((2, 2, 72, LANES), f32),
                pltpu.VMEM((2, 2, 2, 32, LANES), f32),
                pltpu.VMEM((2, len(SOURCES), NB, LANES), f32),
                pltpu.VMEM((2, 2 * NB, LANES), f32),
                pltpu.VMEM((7, EXT, 3, 2 * NB, LANES), f32),
                pltpu.VMEM((NB, 7, 49, NB, LANES), f32),
                pltpu.VMEM((2, NB, 3, NB, LANES), f32),
                pltpu.VMEM((NB, LANES), f32),
                pltpu.VMEM((2, 1, LANES), f32),
                pltpu.VMEM((32, 1, LANES), f32),
                pltpu.VMEM((8, 1, LANES), f32),
                pltpu.SemaphoreType.DMA((2, len(SOURCES))),
                pltpu.SemaphoreType.DMA((2, len(SOURCES))),
                pltpu.SemaphoreType.DMA((2, 32)),
                pltpu.SemaphoreType.DMA((2, 32)),
            ],
            compiler_params=pltpu.CompilerParams(
                collective_id=0,
                has_side_effects=True,
                vmem_limit_bytes=40 * 1024 * 1024,
            ),
        )(*flat)
        shape = displacement.shape
        return (
            newd.reshape(shape),
            newv.reshape(shape),
            newa.reshape(shape),
            energy.reshape(()),
        )

    spec = P(None, "gx", "gz", "gy")
    return jax.shard_map(
        step,
        mesh=mesh,
        in_specs=(spec,) * 4,
        out_specs=(spec,) * 3 + (P(),),
        check_vma=False,
    )
```

```python
import functools
import math

import jax
import jax.numpy as jnp
from jax import lax
from jax.experimental import pallas as pl
from jax.experimental.pallas import tpu as pltpu
from jax.sharding import PartitionSpec as P

MESH = pl.DeviceIdType.MESH
TIME_STEP = 0.05
BITS_PER_WORD = 30
SIDE_X = 4
R = 3
NB = 8
EXT = NB + 2 * R
LANES = 128
REACH = range(-R, R + 1)

FAR = [
    (ez, ex, ey) for ez in (-1, 1) for ex in (0, -1, 1) for ey in (0, -1, 1)
]
NEAR = [(0, ex, ey) for ex in (0, -1, 1) for ey in (0, -1, 1) if (ex, ey) != (0, 0)]
YSLOT = {(ex, ey): i for i, (ex, ey) in enumerate((x, y) for x in (0, -1, 1) for y in (-1, 1))}

CLASSES = {}
for _p in REACH:
    for _r in REACH:
        CLASSES.setdefault(_p * _p + _r * _r, []).append((_p, _r))
CLASSES = sorted(CLASSES.items())


def side(e):
    return 0 if e < 0 else 1


def bond_number(p, q, r):
    flat = (p + R) * 49 + (q + R) * 7 + (r + R)
    return flat if flat < 171 else flat - 1


def weight(p, q, r):
    return 4.0 * math.exp(-(p * p + q * q + r * r) / 9.0)


def kernel(
    sizes,
    disp_hbm,
    vel_hbm,
    body_hbm,
    broken_hbm,
    newd_out,
    newv_out,
    newa_out,
    energy_out,
    disp,
    vel,
    body,
    broken,
    core,
    xpack,
    xrecv,
    ypack,
    yall,
    ynear,
    yfar,
    zrecv,
    zxpack,
    zxrecv,
    yext,
    ext,
    bonds,
    force,
    esum,
    erow,
    eplane,
    ecol,
    load_sem,
    near_send,
    near_recv,
    far_send,
    far_recv,
    esend_sem,
    erecv_sem,
):
    n_gx, n_gy, n_gz = sizes
    gx, gy, gz = lax.axis_index("gx"), lax.axis_index("gy"), lax.axis_index("gz")
    has_low, has_high = gz > 0, gz < n_gz - 1

    def at(ez, ex, ey):
        return (
            lax.rem(gx + ex + n_gx, n_gx),
            lax.rem(gy + ey + n_gy, n_gy),
            gz + ez,
        )

    side_x = SIDE_X
    n_plane = side_x * n_gy * 2
    n_col = (n_gx // side_x) * (n_gz // 2)
    my_x, my_zlo = lax.rem(gx, side_x), gx // side_x
    my_core, my_zhi = lax.rem(gz, 2), gz // 2
    my_plane = (my_x * n_gy + gy) * 2 + my_core
    my_col = my_zhi * (n_gx // side_x) + my_zlo

    def plane_device(m):
        return (
            my_zlo * side_x + m // (2 * n_gy),
            lax.rem(m // 2, n_gy),
            my_zhi * 2 + lax.rem(m, 2),
        )

    def col_device(m):
        return (
            lax.rem(m, n_gx // side_x) * side_x + my_x,
            gy,
            (m // (n_gx // side_x)) * 2 + my_core,
        )

    barrier = pltpu.get_barrier_semaphore()

    def greet(device):
        pl.semaphore_signal(barrier, inc=1, device_id=device, device_id_type=MESH)

    for present, low in ((has_low, True), (has_high, False)):

        @pl.when(present)
        def _(low=low):
            for e in FAR:
                if (e[0] < 0) == low:
                    greet(at(*e))

    for e in NEAR:
        greet(at(*e))

    @pl.loop(1, n_plane)
    def _(j):
        greet(plane_device(lax.rem(my_plane + j, n_plane)))

    @pl.loop(1, n_col)
    def _(j):
        greet(col_device(lax.rem(my_col + j, n_col)))

    loads = [
        pltpu.make_async_copy(src, dst, load_sem.at[i])
        for i, (src, dst) in enumerate(
            ((disp_hbm, disp), (broken_hbm, broken), (vel_hbm, vel), (body_hbm, body))
        )
    ]
    for load in loads:
        load.start()

    lane = lax.broadcasted_iota(jnp.int32, (NB, LANES), 1)
    lane2 = lax.broadcasted_iota(jnp.int32, (2 * NB, LANES), 1)

    for present, low in ((has_low, True), (has_high, False)):

        @pl.when(jnp.logical_not(present))
        def _(low=low):
            s = 0 if low else 1
            for step in (0, 1):
                zrecv[step, s] = jnp.zeros(zrecv.shape[2:], jnp.float32)
                zxrecv[step, s] = jnp.zeros(zxrecv.shape[2:], jnp.float32)
                yfar[step, s] = jnp.zeros(yfar.shape[2:], jnp.float32)

    def near_message(step, e, h):
        _, ex, ey = e
        if ey != 0:
            src = yall.at[0, side(ey)] if step == 0 else ypack.at[h, side(ey)]
            dst = ynear.at[step, YSLOT[ex, ey], h]
        elif step == 0:
            src, dst = xpack.at[0, side(ex)], xrecv.at[0, side(ex)]
        else:
            src, dst = xpack.at[1, side(ex), h], xrecv.at[1, side(ex), h]
        return pltpu.make_async_remote_copy(
            src_ref=src,
            dst_ref=dst,
            send_sem=near_send.at[step, NEAR.index(e), h],
            recv_sem=near_recv.at[step, NEAR.index(e), h],
            device_id=at(0, -ex, -ey),
            device_id_type=MESH,
        )

    def far_message(step, e):
        ez, ex, ey = e
        if ey != 0:
            src = yall.at[step, side(ey)]
            dst = yfar.at[step, side(ez), YSLOT[ex, ey]]
        elif ex == 0:
            src = core.at[step, pl.ds(NB - R if ez < 0 else 0, R)]
            dst = zrecv.at[step, side(ez)]
        else:
            src = zxpack.at[step, side(ez), side(ex)]
            dst = zxrecv.at[step, side(ez), side(ex)]
        return pltpu.make_async_remote_copy(
            src_ref=src,
            dst_ref=dst,
            send_sem=far_send.at[step, FAR.index(e)],
            recv_sem=far_recv.at[step, FAR.index(e)],
            device_id=at(-ez, -ex, -ey),
            device_id_type=MESH,
        )

    def for_far(step, present_below, present_above, act):
        for present, below in ((present_below, True), (present_above, False)):

            @pl.when(present)
            def _(below=below):
                for e in FAR:
                    if (e[0] < 0) == below:
                        act(far_message(step, e))

    def send_far(step):
        for_far(step, has_high, has_low, lambda m: m.start())

    def receive_far(step):
        for_far(step, has_low, has_high, lambda m: m.wait_recv())

    def finish_far(step):
        for_far(step, has_high, has_low, lambda m: m.wait_send())

    def pack_pair(step, h):
        ylow, yhigh = yall[step, 0], yall[step, 1]
        for i, z in enumerate((h, NB - 1 - h)):
            for c in range(3):
                g = 3 * (z * 3 + c)
                k = 3 * (i * 3 + c)
                value = core[step, z, c]
                xpack[step, 0, h, k : k + R, :] = core[step, z, c, NB - R : NB, :]
                xpack[step, 1, h, k : k + R, :] = core[step, z, c, 0:R, :]
                mine = (lane >= g) & (lane < g + R)
                ylow = jnp.where(mine, pltpu.roll(value, g + R, 1), ylow)
                yhigh = jnp.where(mine, pltpu.roll(value, g, 1), yhigh)
        yall[step, 0] = ylow
        yall[step, 1] = yhigh
        if step == 1:
            ypack[h, 0] = ylow
            ypack[h, 1] = yhigh

    def pack_far(step):
        for s, base in ((0, NB - R), (1, 0)):
            for i in range(R):
                for c in range(3):
                    k = 3 * (i * 3 + c)
                    zxpack[step, s, 0, k : k + R, :] = core[
                        step, base + i, c, NB - R : NB, :
                    ]
                    zxpack[step, s, 1, k : k + R, :] = core[step, base + i, c, 0:R, :]

    def shift_row(slot, row, z):
        for c in range(3):
            g = 3 * (z * 3 + c)
            left = pltpu.roll(yext[slot, 0], LANES - R - g, 1)
            right = pltpu.roll(yext[slot, 1], lax.rem(LANES - g, LANES), 1)
            here = ext[R, row, c]
            for r in range(1, R + 1):
                ext[R + r, row, c] = pltpu.roll(
                    jnp.where(lane2 < r, right, here), LANES - r, 1
                )
                ext[R - r, row, c] = pltpu.roll(
                    jnp.where(lane2 >= LANES - r, left, here), r, 1
                )

    def fill_pair(step, h):
        held = 0 if step == 0 else h
        for s, ey in ((0, -1), (1, 1)):
            yext[0, s, R : R + NB, :] = ynear[step, YSLOT[0, ey], held]
            yext[0, s, 0:R, :] = ynear[step, YSLOT[-1, ey], held, NB - R : NB, :]
            yext[0, s, R + NB : EXT, :] = ynear[step, YSLOT[1, ey], held, 0:R, :]
        for i, z in enumerate((h, NB - 1 - h)):
            for c in range(3):
                k = 3 * (i * 3 + c)
                ext[R, z + R, c, R : R + NB, :] = core[step, z, c]
                for s, row in ((0, 0), (1, R + NB)):
                    ext[R, z + R, c, row : row + R, :] = xrecv[
                        step, s, h, k : k + R, :
                    ]
        for z in (h, NB - 1 - h):
            shift_row(0, z + R, z)

    def fill_far(step):
        for zs, first in ((0, 0), (1, R + NB)):
            for i in range(R):
                for c in range(3):
                    k = 3 * (i * 3 + c)
                    ext[R, first + i, c, R : R + NB, :] = zrecv[step, zs, i, c]
                    for s, row in ((0, 0), (1, R + NB)):
                        ext[R, first + i, c, row : row + R, :] = zxrecv[
                            step, zs, s, k : k + R, :
                        ]
            for s, ey in ((0, -1), (1, 1)):
                yext[zs, s, R : R + NB, :] = yfar[step, zs, YSLOT[0, ey]]
                yext[zs, s, 0:R, :] = yfar[step, zs, YSLOT[-1, ey], NB - R : NB, :]
                yext[zs, s, R + NB : EXT, :] = yfar[step, zs, YSLOT[1, ey], 0:R, :]

        @pl.loop(0, R)
        def _(i):
            shift_row(0, i, NB - R + i)
            shift_row(1, R + NB + i, i)

    def unpack_bonds():
        @pl.loop(0, NB)
        def _(z):
            words = [broken[w, pl.ds(z, NB, stride=NB), :] for w in range(12)]
            depth = gz * NB + z
            for q in REACH:
                inside = (depth + q >= 0) & (depth + q < n_gz * NB)
                scale = jnp.where(inside, 1.0, 0.0)
                for _, members in CLASSES:
                    whole = jnp.full(
                        (NB, LANES), scale * weight(members[0][0], q, members[0][1])
                    )
                    for p, r in members:
                        j = (p + R) * 7 + r + R
                        if (p, q, r) == (0, 0, 0):
                            bonds[z, q + R, j] = jnp.zeros((NB, LANES), jnp.float32)
                            continue
                        k = bond_number(p, q, r)
                        bit = words[k // BITS_PER_WORD] & (1 << (k % BITS_PER_WORD))
                        bonds[z, q + R, j] = jnp.where(bit == 0, whole, 0.0)

    def add_row(step, z, q, task):
        cx, cz, cy = (core[step, z, c] for c in range(3))
        cz = cz - q.astype(jnp.float32)
        cxs = {p: cx - float(p) if p else cx for p in REACH}
        cys = {r: cy - float(r) if r else cy for r in REACH}
        row = z + q + R
        fx = fz = fy = energy = None

        def plus(a, b):
            return b if a is None else a + b

        for square, members in CLASSES:
            own = jnp.where(q == 0, 1, 0) if square == 0 else 0
            rest_square = (q * q + square + own).astype(jnp.float32)
            if task != "pull":
                inverse_rest = lax.rsqrt(jnp.full((NB, LANES), rest_square))
            class_energy = None
            for p, r in members:
                there = ext.at[r + R, row]
                j = (p + R) * 7 + r + R
                bx = there[0, R + p : R + p + NB, :] - cxs[p]
                bz = there[1, R + p : R + p + NB, :] - cz
                by = there[2, R + p : R + p + NB, :] - cys[r]
                pull = bonds[z, q + R, j]
                if task != "pull":
                    length_square = bx * bx + bz * bz + by * by
                    if square == 0:
                        length_square = length_square + own.astype(jnp.float32)
                    gap = inverse_rest - lax.rsqrt(length_square)
                    pull = pull * gap
                if task == "energy":
                    bonds[z, q + R, j] = pull
                    class_energy = plus(class_energy, pull * gap * length_square)
                else:
                    fx = plus(fx, pull * bx)
                    fz = plus(fz, pull * bz)
                    fy = plus(fy, pull * by)
            if task == "energy":
                rest = jnp.full((NB, LANES), rest_square) * inverse_rest
                energy = plus(energy, class_energy * rest)
        if task == "energy":
            return energy
        force[step, z, 0] += fx
        force[step, z, 1] += fz
        force[step, z, 2] += fy

    def add_pair(step, z, q, task):
        first = add_row(step, z, q, task)
        second = add_row(step, NB - 1 - z, -q, task)
        if task == "energy":
            esum[...] += first + second

    def phase(turn):
        return lax.rem(turn + NB // 2 - 1, NB // 2)

    loads[0].wait()
    for step in (0, 1):
        yall[step] = jnp.zeros(yall.shape[1:], jnp.float32)
        for s in (0, 1):
            for h in range(NB // 2):
                xpack[step, s, h, 16:24, :] = jnp.zeros((NB, LANES), jnp.float32)
            for t in (0, 1):
                zxpack[step, s, t, 24:32, :] = jnp.zeros((NB, LANES), jnp.float32)

    @pl.loop(0, NB // 2)
    def _(h):
        for z in (h, NB - 1 - h):
            for c in range(3):
                core[0, z, c] = disp[c, pl.ds(z, NB, stride=NB), :]
        pack_pair(0, h)

    pack_far(0)
    half = len(FAR) // 2
    greeted = (
        len(NEAR)
        + half * (jnp.where(has_low, 1, 0) + jnp.where(has_high, 1, 0))
        + (n_plane - 1)
        + (n_col - 1)
    )
    pl.semaphore_wait(barrier, greeted)
    send_far(0)
    for e in NEAR:
        near_message(0, e, 0).start()

    for load in loads[1:]:
        load.wait()
    unpack_bonds()
    esum[...] = jnp.zeros((NB, LANES), jnp.float32)

    @pl.loop(0, NB)
    def _(z):
        for c in range(3):
            value = body[c, pl.ds(z, NB, stride=NB), :]
            force[0, z, c] = value
            force[1, z, c] = value

    for e in NEAR:
        near_message(0, e, 0).wait_recv()

    @pl.loop(0, NB // 2)
    def _(h):
        fill_pair(0, h)

    @pl.loop(0, NB // 2)
    def _(turn):
        h = phase(turn)

        @pl.when(turn == 1)
        def _():
            receive_far(0)
            fill_far(0)

        @pl.loop(0, 2 * R + 1)
        def _(place):
            add_pair(0, h, place - R, "force")

        for z in (h, NB - 1 - h):
            for c in range(3):
                rows = pl.ds(z, NB, stride=NB)
                moved = (
                    core[0, z, c]
                    + TIME_STEP * vel[c, rows, :]
                    + (0.5 * TIME_STEP * TIME_STEP) * force[0, z, c]
                )
                core[1, z, c] = moved
                newd_out[c, rows, :] = moved
        pack_pair(1, h)
        for e in NEAR:
            near_message(1, e, h).start()

    pack_far(1)
    send_far(1)

    @pl.loop(0, NB // 2)
    def _(turn):
        h = phase(turn)
        for e in NEAR:
            near_message(1, e, h).wait_recv()
        fill_pair(1, h)

        @pl.loop(0, h + R + 1)
        def _(z):
            add_pair(1, z, h - z, "energy")

    receive_far(1)
    fill_far(1)

    @pl.loop(1, R + 1)
    def _(q):
        @pl.loop(NB - q, NB)
        def _(z):
            add_pair(1, z, q, "energy")

    erow[0] = jnp.sum(esum[...], axis=0, keepdims=True)
    eplane[my_plane] = erow[0]

    def plane_message(j, slot, device):
        return pltpu.make_async_remote_copy(
            src_ref=erow.at[0],
            dst_ref=eplane.at[slot],
            send_sem=esend_sem.at[0, j],
            recv_sem=erecv_sem.at[0, j],
            device_id=plane_device(device),
            device_id_type=MESH,
        )

    @pl.loop(1, n_plane)
    def _(j):
        plane_message(j, my_plane, lax.rem(my_plane + j, n_plane)).start()

    @pl.loop(0, NB // 2)
    def _(h):
        @pl.loop(0, 2 * R + 1)
        def _(place):
            add_pair(1, h, place - R, "pull")

        for z in (h, NB - 1 - h):
            for c in range(3):
                rows = pl.ds(z, NB, stride=NB)
                newa = force[1, z, c]
                newa_out[c, rows, :] = newa
                newv_out[c, rows, :] = vel[c, rows, :] + (0.5 * TIME_STEP) * (
                    force[0, z, c] + newa
                )

    @pl.loop(1, n_plane)
    def _(j):
        other = lax.rem(my_plane - j + n_plane, n_plane)
        plane_message(j, other, other).wait()

    total = eplane[0]
    for m in range(1, n_plane):
        total = total + eplane[m]
    erow[1] = total
    ecol[my_col] = total

    def col_message(j, slot, device):
        return pltpu.make_async_remote_copy(
            src_ref=erow.at[1],
            dst_ref=ecol.at[slot],
            send_sem=esend_sem.at[1, j],
            recv_sem=erecv_sem.at[1, j],
            device_id=col_device(device),
            device_id_type=MESH,
        )

    @pl.loop(1, n_col)
    def _(j):
        col_message(j, my_col, lax.rem(my_col + j, n_col)).start()

    for e in NEAR:
        near_message(0, e, 0).wait_send()

    @pl.loop(0, NB // 2)
    def _(h):
        for e in NEAR:
            near_message(1, e, h).wait_send()

    finish_far(0)
    finish_far(1)

    @pl.loop(1, n_col)
    def _(j):
        other = lax.rem(my_col - j + n_col, n_col)
        col_message(j, other, other).wait()

    total = ecol[0]
    for m in range(1, n_col):
        total = total + ecol[m]
    area = (n_gx * NB) * (n_gy * LANES)
    energy_out[0, 0] = jnp.sum(total) * (0.25 / area)


def solution(mesh):
    sizes = (mesh.shape["gx"], mesh.shape["gy"], mesh.shape["gz"])
    f32 = jnp.float32
    block = jax.ShapeDtypeStruct((3, NB * NB, LANES), f32)

    def step(displacement, velocity, body_force, broken):
        flat = [
            a.reshape(a.shape[0], NB * NB, LANES)
            for a in (displacement, velocity, body_force, broken)
        ]
        newd, newv, newa, energy = pl.pallas_call(
            functools.partial(kernel, sizes),
            out_shape=(block, block, block, jax.ShapeDtypeStruct((1, 1), f32)),
            in_specs=[pl.BlockSpec(memory_space=pl.ANY)] * 4,
            out_specs=[pl.BlockSpec(memory_space=pltpu.VMEM)] * 3
            + [pl.BlockSpec(memory_space=pltpu.SMEM)],
            scratch_shapes=[
                pltpu.VMEM((3, NB * NB, LANES), f32),
                pltpu.VMEM((3, NB * NB, LANES), f32),
                pltpu.VMEM((3, NB * NB, LANES), f32),
                pltpu.VMEM((12, NB * NB, LANES), jnp.int32),
                pltpu.VMEM((2, NB, 3, NB, LANES), f32),
                pltpu.VMEM((2, 2, NB // 2, 24, LANES), f32),
                pltpu.VMEM((2, 2, NB // 2, 24, LANES), f32),
                pltpu.VMEM((NB // 2, 2, NB, LANES), f32),
                pltpu.VMEM((2, 2, NB, LANES), f32),
                pltpu.VMEM((2, 6, NB // 2, NB, LANES), f32),
                pltpu.VMEM((2, 2, 6, NB, LANES), f32),
                pltpu.VMEM((2, 2, R, 3, NB, LANES), f32),
                pltpu.VMEM((2, 2, 2, 32, LANES), f32),
                pltpu.VMEM((2, 2, 2, 32, LANES), f32),
                pltpu.VMEM((2, 2, 2 * NB, LANES), f32),
                pltpu.VMEM((7, EXT, 3, 2 * NB, LANES), f32),
                pltpu.VMEM((NB, 7, 49, NB, LANES), f32),
                pltpu.VMEM((2, NB, 3, NB, LANES), f32),
                pltpu.VMEM((NB, LANES), f32),
                pltpu.VMEM((2, 1, LANES), f32),
                pltpu.VMEM((32, 1, LANES), f32),
                pltpu.VMEM((8, 1, LANES), f32),
                pltpu.SemaphoreType.DMA((4,)),
                pltpu.SemaphoreType.DMA((2, len(NEAR), NB // 2)),
                pltpu.SemaphoreType.DMA((2, len(NEAR), NB // 2)),
                pltpu.SemaphoreType.DMA((2, len(FAR))),
                pltpu.SemaphoreType.DMA((2, len(FAR))),
                pltpu.SemaphoreType.DMA((2, 32)),
                pltpu.SemaphoreType.DMA((2, 32)),
            ],
            compiler_params=pltpu.CompilerParams(
                collective_id=0,
                has_side_effects=True,
                vmem_limit_bytes=66_700_000,
            ),
        )(*flat)
        shape = displacement.shape
        return (
            newd.reshape(shape),
            newv.reshape(shape),
            newa.reshape(shape),
            energy.reshape(()),
        )

    spec = P(None, "gx", "gz", "gy")
    return jax.shard_map(
        step,
        mesh=mesh,
        in_specs=(spec,) * 4,
        out_specs=(spec,) * 3 + (P(),),
        check_vma=False,
    )
```

```python
import functools
import math

import jax
import jax.numpy as jnp
from jax import lax
from jax.experimental import pallas as pl
from jax.experimental.pallas import tpu as pltpu
from jax.sharding import PartitionSpec as P

MESH = pl.DeviceIdType.MESH
TIME_STEP = 0.05
BITS_PER_WORD = 30
SIDE_X = 4
R = 3
NB = 8
EXT = NB + 2 * R
LANES = 128
REACH = range(-R, R + 1)

FAR = [
    (ez, ex, ey) for ez in (-1, 1) for ex in (0, -1, 1) for ey in (0, -1, 1)
]
NEAR = [(0, ex, ey) for ex in (0, -1, 1) for ey in (0, -1, 1) if (ex, ey) != (0, 0)]
YSLOT = {(ex, ey): i for i, (ex, ey) in enumerate((x, y) for x in (0, -1, 1) for y in (-1, 1))}

CLASSES = {}
for _p in REACH:
    for _r in REACH:
        CLASSES.setdefault(_p * _p + _r * _r, []).append((_p, _r))
CLASSES = sorted(CLASSES.items())


def side(e):
    return 0 if e < 0 else 1


def bond_number(p, q, r):
    flat = (p + R) * 49 + (q + R) * 7 + (r + R)
    return flat if flat < 171 else flat - 1


def weight(p, q, r):
    return 4.0 * math.exp(-(p * p + q * q + r * r) / 9.0)


def kernel(
    sizes,
    disp_hbm,
    vel_hbm,
    body_hbm,
    broken_hbm,
    newd_out,
    newv_out,
    newa_out,
    energy_out,
    disp,
    vel,
    body,
    broken,
    core,
    xpack,
    xrecv,
    ypack,
    yall,
    ynear,
    yfar,
    zrecv,
    zxpack,
    zxrecv,
    yext,
    ext,
    bonds,
    force,
    esum,
    erow,
    eplane,
    ecol,
    load_sem,
    near_send,
    near_recv,
    far_send,
    far_recv,
    esend_sem,
    erecv_sem,
):
    n_gx, n_gy, n_gz = sizes
    gx, gy, gz = lax.axis_index("gx"), lax.axis_index("gy"), lax.axis_index("gz")
    has_low, has_high = gz > 0, gz < n_gz - 1

    def at(ez, ex, ey):
        return (
            lax.rem(gx + ex + n_gx, n_gx),
            lax.rem(gy + ey + n_gy, n_gy),
            gz + ez,
        )

    side_x = SIDE_X
    n_plane = side_x * n_gy * 2
    n_col = (n_gx // side_x) * (n_gz // 2)
    my_x, my_zlo = lax.rem(gx, side_x), gx // side_x
    my_core, my_zhi = lax.rem(gz, 2), gz // 2
    my_plane = (my_x * n_gy + gy) * 2 + my_core
    my_col = my_zhi * (n_gx // side_x) + my_zlo

    def plane_device(m):
        return (
            my_zlo * side_x + m // (2 * n_gy),
            lax.rem(m // 2, n_gy),
            my_zhi * 2 + lax.rem(m, 2),
        )

    def col_device(m):
        return (
            lax.rem(m, n_gx // side_x) * side_x + my_x,
            gy,
            (m // (n_gx // side_x)) * 2 + my_core,
        )

    barrier = pltpu.get_barrier_semaphore()

    def greet(device):
        pl.semaphore_signal(barrier, inc=1, device_id=device, device_id_type=MESH)

    for present, low in ((has_low, True), (has_high, False)):

        @pl.when(present)
        def _(low=low):
            for e in FAR:
                if (e[0] < 0) == low:
                    greet(at(*e))

    for e in NEAR:
        greet(at(*e))

    @pl.loop(1, n_plane)
    def _(j):
        greet(plane_device(lax.rem(my_plane + j, n_plane)))

    @pl.loop(1, n_col)
    def _(j):
        greet(col_device(lax.rem(my_col + j, n_col)))

    loads = [
        pltpu.make_async_copy(src, dst, load_sem.at[i])
        for i, (src, dst) in enumerate(
            ((disp_hbm, disp), (broken_hbm, broken), (vel_hbm, vel), (body_hbm, body))
        )
    ]
    for load in loads:
        load.start()

    lane = lax.broadcasted_iota(jnp.int32, (NB, LANES), 1)
    lane2 = lax.broadcasted_iota(jnp.int32, (2 * NB, LANES), 1)
    middle = 0.5 * (NB - 1)
    place = lax.broadcasted_iota(jnp.int32, (NB, LANES), 0).astype(jnp.float32) - middle
    place2 = lax.broadcasted_iota(jnp.int32, (2 * NB, LANES), 0).astype(
        jnp.float32
    ) - (middle + R)

    for present, low in ((has_low, True), (has_high, False)):

        @pl.when(jnp.logical_not(present))
        def _(low=low):
            s = 0 if low else 1
            for step in (0, 1):
                zrecv[step, s] = jnp.zeros(zrecv.shape[2:], jnp.float32)
                zxrecv[step, s] = jnp.zeros(zxrecv.shape[2:], jnp.float32)
                yfar[step, s] = jnp.zeros(yfar.shape[2:], jnp.float32)

    def near_message(step, e, h):
        _, ex, ey = e
        if ey != 0:
            src = yall.at[0, side(ey)] if step == 0 else ypack.at[h, side(ey)]
            dst = ynear.at[step, YSLOT[ex, ey], h]
        elif step == 0:
            src, dst = xpack.at[0, side(ex)], xrecv.at[0, side(ex)]
        else:
            src, dst = xpack.at[1, side(ex), h], xrecv.at[1, side(ex), h]
        return pltpu.make_async_remote_copy(
            src_ref=src,
            dst_ref=dst,
            send_sem=near_send.at[step, NEAR.index(e), h],
            recv_sem=near_recv.at[step, NEAR.index(e), h],
            device_id=at(0, -ex, -ey),
            device_id_type=MESH,
        )

    def far_message(step, e):
        ez, ex, ey = e
        if ey != 0:
            src = yall.at[step, side(ey)]
            dst = yfar.at[step, side(ez), YSLOT[ex, ey]]
        elif ex == 0:
            src = core.at[step, pl.ds(NB - R if ez < 0 else 0, R)]
            dst = zrecv.at[step, side(ez)]
        else:
            src = zxpack.at[step, side(ez), side(ex)]
            dst = zxrecv.at[step, side(ez), side(ex)]
        return pltpu.make_async_remote_copy(
            src_ref=src,
            dst_ref=dst,
            send_sem=far_send.at[step, FAR.index(e)],
            recv_sem=far_recv.at[step, FAR.index(e)],
            device_id=at(-ez, -ex, -ey),
            device_id_type=MESH,
        )

    def for_far(step, present_below, present_above, act):
        for present, below in ((present_below, True), (present_above, False)):

            @pl.when(present)
            def _(below=below):
                for e in FAR:
                    if (e[0] < 0) == below:
                        act(far_message(step, e))

    def send_far(step):
        for_far(step, has_high, has_low, lambda m: m.start())

    def receive_far(step):
        for_far(step, has_low, has_high, lambda m: m.wait_recv())

    def finish_far(step):
        for_far(step, has_high, has_low, lambda m: m.wait_send())

    def pack_pair(step, h):
        ylow, yhigh = yall[step, 0], yall[step, 1]
        for i, z in enumerate((h, NB - 1 - h)):
            for c in range(3):
                g = 3 * (z * 3 + c)
                k = 3 * (i * 3 + c)
                value = core[step, z, c]
                xpack[step, 0, h, k : k + R, :] = core[step, z, c, NB - R : NB, :]
                xpack[step, 1, h, k : k + R, :] = core[step, z, c, 0:R, :]
                mine = (lane >= g) & (lane < g + R)
                ylow = jnp.where(mine, pltpu.roll(value, g + R, 1), ylow)
                yhigh = jnp.where(mine, pltpu.roll(value, g, 1), yhigh)
        yall[step, 0] = ylow
        yall[step, 1] = yhigh
        if step == 1:
            ypack[h, 0] = ylow
            ypack[h, 1] = yhigh

    def pack_far(step):
        for s, base in ((0, NB - R), (1, 0)):
            for i in range(R):
                for c in range(3):
                    k = 3 * (i * 3 + c)
                    zxpack[step, s, 0, k : k + R, :] = core[
                        step, base + i, c, NB - R : NB, :
                    ]
                    zxpack[step, s, 1, k : k + R, :] = core[step, base + i, c, 0:R, :]

    def shift_rows(rows):
        strips = {slot: (yext[slot, 0], yext[slot, 1]) for slot, _, _ in rows}
        here = [[ext[R, row, c] for c in range(3)] for _, row, _ in rows]
        for (slot, row, z), values in zip(rows, here):
            for c in range(3):
                g = 3 * (z * 3 + c)
                left = pltpu.roll(strips[slot][0], LANES - R - g, 1)
                right = pltpu.roll(strips[slot][1], lax.rem(LANES - g, LANES), 1)
                value = values[c]
                if c == 0:
                    left, right, value = left + place2, right + place2, value + place2
                    ext[R, row, c] = value
                for r in range(1, R + 1):
                    after = pltpu.roll(
                        jnp.where(lane2 < r, right, value), LANES - r, 1
                    )
                    before = pltpu.roll(
                        jnp.where(lane2 >= LANES - r, left, value), r, 1
                    )
                    if c == 2:
                        after, before = after + float(r), before - float(r)
                    ext[R + r, row, c] = after
                    ext[R - r, row, c] = before

    def fill_pair(step, h):
        held = 0 if step == 0 else h
        for s, ey in ((0, -1), (1, 1)):
            yext[0, s, R : R + NB, :] = ynear[step, YSLOT[0, ey], held]
            yext[0, s, 0:R, :] = ynear[step, YSLOT[-1, ey], held, NB - R : NB, :]
            yext[0, s, R + NB : EXT, :] = ynear[step, YSLOT[1, ey], held, 0:R, :]
        for i, z in enumerate((h, NB - 1 - h)):
            for c in range(3):
                k = 3 * (i * 3 + c)
                ext[R, z + R, c, R : R + NB, :] = core[step, z, c]
                for s, row in ((0, 0), (1, R + NB)):
                    ext[R, z + R, c, row : row + R, :] = xrecv[
                        step, s, h, k : k + R, :
                    ]
        shift_rows([(0, z + R, z) for z in (h, NB - 1 - h)])

    def fill_far(step):
        for zs, first in ((0, 0), (1, R + NB)):
            for i in range(R):
                for c in range(3):
                    k = 3 * (i * 3 + c)
                    ext[R, first + i, c, R : R + NB, :] = zrecv[step, zs, i, c]
                    for s, row in ((0, 0), (1, R + NB)):
                        ext[R, first + i, c, row : row + R, :] = zxrecv[
                            step, zs, s, k : k + R, :
                        ]
            for s, ey in ((0, -1), (1, 1)):
                yext[zs, s, R : R + NB, :] = yfar[step, zs, YSLOT[0, ey]]
                yext[zs, s, 0:R, :] = yfar[step, zs, YSLOT[-1, ey], NB - R : NB, :]
                yext[zs, s, R + NB : EXT, :] = yfar[step, zs, YSLOT[1, ey], 0:R, :]

        @pl.loop(0, R)
        def _(i):
            shift_rows([(0, i, NB - R + i), (1, R + NB + i, i)])

    def unpack_bonds():
        @pl.loop(0, NB)
        def _(z):
            words = [broken[w, pl.ds(z, NB, stride=NB), :] for w in range(12)]
            depth = gz * NB + z
            for q in REACH:
                inside = (depth + q >= 0) & (depth + q < n_gz * NB)
                scale = jnp.where(inside, 1.0, 0.0)
                for _, members in CLASSES:
                    whole = jnp.full(
                        (NB, LANES), scale * weight(members[0][0], q, members[0][1])
                    )
                    for p, r in members:
                        j = (p + R) * 7 + r + R
                        if (p, q, r) == (0, 0, 0):
                            bonds[z, q + R, j] = jnp.zeros((NB, LANES), jnp.float32)
                            continue
                        k = bond_number(p, q, r)
                        bit = words[k // BITS_PER_WORD] & (1 << (k % BITS_PER_WORD))
                        bonds[z, q + R, j] = jnp.where(bit == 0, whole, 0.0)

    def add_row(step, z, q, task):
        cx, cz, cy = (core[step, z, c] for c in range(3))
        cx = cx + place
        cz = cz - q.astype(jnp.float32)
        row = z + q + R
        fx = fz = fy = energy = None

        def plus(a, b):
            return b if a is None else a + b

        for square, members in CLASSES:
            own = jnp.where(q == 0, 1, 0) if square == 0 else 0
            rest_square = (q * q + square + own).astype(jnp.float32)
            if task != "pull":
                inverse_rest = lax.rsqrt(jnp.full((NB, LANES), rest_square))
            class_energy = None
            for p, r in members:
                there = ext.at[r + R, row]
                j = (p + R) * 7 + r + R
                bx = there[0, R + p : R + p + NB, :] - cx
                bz = there[1, R + p : R + p + NB, :] - cz
                by = there[2, R + p : R + p + NB, :] - cy
                pull = bonds[z, q + R, j]
                if task != "pull":
                    length_square = bx * bx + bz * bz + by * by
                    if square == 0:
                        length_square = length_square + own.astype(jnp.float32)
                    gap = inverse_rest - lax.rsqrt(length_square)
                    pull = pull * gap
                if task == "energy":
                    bonds[z, q + R, j] = pull
                    class_energy = plus(class_energy, pull * gap * length_square)
                else:
                    fx = plus(fx, pull * bx)
                    fz = plus(fz, pull * bz)
                    fy = plus(fy, pull * by)
            if task == "energy":
                rest = jnp.full((NB, LANES), rest_square) * inverse_rest
                energy = plus(energy, class_energy * rest)
        if task == "energy":
            return energy
        force[step, z, 0] += fx
        force[step, z, 1] += fz
        force[step, z, 2] += fy

    def add_pair(step, z, q, task):
        first = add_row(step, z, q, task)
        second = add_row(step, NB - 1 - z, -q, task)
        if task == "energy":
            esum[...] += first + second

    def phase(turn):
        return lax.rem(turn + NB // 2 - 1, NB // 2)

    loads[0].wait()
    for step in (0, 1):
        yall[step] = jnp.zeros(yall.shape[1:], jnp.float32)
        for s in (0, 1):
            for h in range(NB // 2):
                xpack[step, s, h, 16:24, :] = jnp.zeros((NB, LANES), jnp.float32)
            for t in (0, 1):
                zxpack[step, s, t, 24:32, :] = jnp.zeros((NB, LANES), jnp.float32)

    @pl.loop(0, NB // 2)
    def _(h):
        for z in (h, NB - 1 - h):
            for c in range(3):
                core[0, z, c] = disp[c, pl.ds(z, NB, stride=NB), :]
        pack_pair(0, h)

    pack_far(0)
    half = len(FAR) // 2
    greeted = (
        len(NEAR)
        + half * (jnp.where(has_low, 1, 0) + jnp.where(has_high, 1, 0))
        + (n_plane - 1)
        + (n_col - 1)
    )
    pl.semaphore_wait(barrier, greeted)
    send_far(0)
    for e in NEAR:
        near_message(0, e, 0).start()

    for load in loads[1:]:
        load.wait()
    unpack_bonds()
    esum[...] = jnp.zeros((NB, LANES), jnp.float32)

    @pl.loop(0, NB)
    def _(z):
        for c in range(3):
            value = body[c, pl.ds(z, NB, stride=NB), :]
            force[0, z, c] = value
            force[1, z, c] = value

    for e in NEAR:
        near_message(0, e, 0).wait_recv()

    @pl.loop(0, NB // 2)
    def _(h):
        fill_pair(0, h)

    @pl.loop(0, NB // 2)
    def _(turn):
        h = phase(turn)

        @pl.when(turn == 1)
        def _():
            receive_far(0)
            fill_far(0)

        @pl.loop(0, 2 * R + 1)
        def _(step_q):
            add_pair(0, h, step_q - R, "force")

        for z in (h, NB - 1 - h):
            for c in range(3):
                rows = pl.ds(z, NB, stride=NB)
                moved = (
                    core[0, z, c]
                    + TIME_STEP * vel[c, rows, :]
                    + (0.5 * TIME_STEP * TIME_STEP) * force[0, z, c]
                )
                core[1, z, c] = moved
                newd_out[c, rows, :] = moved
        pack_pair(1, h)
        for e in NEAR:
            near_message(1, e, h).start()

    pack_far(1)
    send_far(1)

    @pl.loop(0, NB // 2)
    def _(turn):
        h = phase(turn)
        for e in NEAR:
            near_message(1, e, h).wait_recv()
        fill_pair(1, h)

        @pl.loop(0, h + R + 1)
        def _(z):
            add_pair(1, z, h - z, "energy")

    receive_far(1)
    fill_far(1)

    @pl.loop(1, R + 1)
    def _(q):
        @pl.loop(NB - q, NB)
        def _(z):
            add_pair(1, z, q, "energy")

    erow[0] = jnp.sum(esum[...], axis=0, keepdims=True)
    eplane[my_plane] = erow[0]

    def plane_message(j, slot, device):
        return pltpu.make_async_remote_copy(
            src_ref=erow.at[0],
            dst_ref=eplane.at[slot],
            send_sem=esend_sem.at[0, j],
            recv_sem=erecv_sem.at[0, j],
            device_id=plane_device(device),
            device_id_type=MESH,
        )

    @pl.loop(1, n_plane)
    def _(j):
        plane_message(j, my_plane, lax.rem(my_plane + j, n_plane)).start()

    @pl.loop(0, NB // 2)
    def _(h):
        @pl.loop(0, 2 * R + 1)
        def _(step_q):
            add_pair(1, h, step_q - R, "pull")

        for z in (h, NB - 1 - h):
            for c in range(3):
                rows = pl.ds(z, NB, stride=NB)
                newa = force[1, z, c]
                newa_out[c, rows, :] = newa
                newv_out[c, rows, :] = vel[c, rows, :] + (0.5 * TIME_STEP) * (
                    force[0, z, c] + newa
                )

    @pl.loop(1, n_plane)
    def _(j):
        other = lax.rem(my_plane - j + n_plane, n_plane)
        plane_message(j, other, other).wait()

    total = eplane[0]
    for m in range(1, n_plane):
        total = total + eplane[m]
    erow[1] = total
    ecol[my_col] = total

    def col_message(j, slot, device):
        return pltpu.make_async_remote_copy(
            src_ref=erow.at[1],
            dst_ref=ecol.at[slot],
            send_sem=esend_sem.at[1, j],
            recv_sem=erecv_sem.at[1, j],
            device_id=col_device(device),
            device_id_type=MESH,
        )

    @pl.loop(1, n_col)
    def _(j):
        col_message(j, my_col, lax.rem(my_col + j, n_col)).start()

    for e in NEAR:
        near_message(0, e, 0).wait_send()

    @pl.loop(0, NB // 2)
    def _(h):
        for e in NEAR:
            near_message(1, e, h).wait_send()

    finish_far(0)
    finish_far(1)

    @pl.loop(1, n_col)
    def _(j):
        other = lax.rem(my_col - j + n_col, n_col)
        col_message(j, other, other).wait()

    total = ecol[0]
    for m in range(1, n_col):
        total = total + ecol[m]
    area = (n_gx * NB) * (n_gy * LANES)
    energy_out[0, 0] = jnp.sum(total) * (0.25 / area)


def hand_out(*refs):
    n = len(refs) // 2
    copies = [
        pltpu.make_async_copy(refs[i], refs[n + i], refs[2 * n].at[i]) for i in range(n)
    ]
    for copy in copies:
        copy.start()
    for copy in copies:
        copy.wait()


def solution(mesh):
    sizes = (mesh.shape["gx"], mesh.shape["gy"], mesh.shape["gz"])
    f32 = jnp.float32
    block = jax.ShapeDtypeStruct((3, NB * NB, LANES), f32)

    def step(displacement, velocity, body_force, broken):
        flat = [
            a.reshape(a.shape[0], NB * NB, LANES)
            for a in (displacement, velocity, body_force, broken)
        ]
        newd, newv, newa, energy = pl.pallas_call(
            functools.partial(kernel, sizes),
            out_shape=(block, block, block, jax.ShapeDtypeStruct((1, 1), f32)),
            in_specs=[pl.BlockSpec(memory_space=pl.ANY)] * 4,
            out_specs=[pl.BlockSpec(memory_space=pltpu.VMEM)] * 3
            + [pl.BlockSpec(memory_space=pltpu.SMEM)],
            scratch_shapes=[
                pltpu.VMEM((3, NB * NB, LANES), f32),
                pltpu.VMEM((3, NB * NB, LANES), f32),
                pltpu.VMEM((3, NB * NB, LANES), f32),
                pltpu.VMEM((12, NB * NB, LANES), jnp.int32),
                pltpu.VMEM((2, NB, 3, NB, LANES), f32),
                pltpu.VMEM((2, 2, NB // 2, 24, LANES), f32),
                pltpu.VMEM((2, 2, NB // 2, 24, LANES), f32),
                pltpu.VMEM((NB // 2, 2, NB, LANES), f32),
                pltpu.VMEM((2, 2, NB, LANES), f32),
                pltpu.VMEM((2, 6, NB // 2, NB, LANES), f32),
                pltpu.VMEM((2, 2, 6, NB, LANES), f32),
                pltpu.VMEM((2, 2, R, 3, NB, LANES), f32),
                pltpu.VMEM((2, 2, 2, 32, LANES), f32),
                pltpu.VMEM((2, 2, 2, 32, LANES), f32),
                pltpu.VMEM((2, 2, 2 * NB, LANES), f32),
                pltpu.VMEM((7, EXT, 3, 2 * NB, LANES), f32),
                pltpu.VMEM((NB, 7, 49, NB, LANES), f32),
                pltpu.VMEM((2, NB, 3, NB, LANES), f32),
                pltpu.VMEM((NB, LANES), f32),
                pltpu.VMEM((2, 1, LANES), f32),
                pltpu.VMEM((32, 1, LANES), f32),
                pltpu.VMEM((8, 1, LANES), f32),
                pltpu.SemaphoreType.DMA((4,)),
                pltpu.SemaphoreType.DMA((2, len(NEAR), NB // 2)),
                pltpu.SemaphoreType.DMA((2, len(NEAR), NB // 2)),
                pltpu.SemaphoreType.DMA((2, len(FAR))),
                pltpu.SemaphoreType.DMA((2, len(FAR))),
                pltpu.SemaphoreType.DMA((2, 32)),
                pltpu.SemaphoreType.DMA((2, 32)),
            ],
            compiler_params=pltpu.CompilerParams(
                collective_id=0,
                has_side_effects=True,
                vmem_limit_bytes=40_000_000,
            ),
        )(*[pltpu.with_memory_space_constraint(a, pltpu.HBM) for a in flat])
        newd, newv, newa = pl.pallas_call(
            hand_out,
            out_shape=(block,) * 3,
            in_specs=[pl.BlockSpec(memory_space=pl.ANY)] * 3,
            out_specs=[pl.BlockSpec(memory_space=pl.ANY)] * 3,
            scratch_shapes=[pltpu.SemaphoreType.DMA((3,))],
            compiler_params=pltpu.CompilerParams(vmem_limit_bytes=40_000_000),
        )(newd, newv, newa)
        shape = displacement.shape
        return (
            newd.reshape(shape),
            newv.reshape(shape),
            newa.reshape(shape),
            energy.reshape(()),
        )

    spec = P(None, "gx", "gz", "gy")
    return jax.shard_map(
        step,
        mesh=mesh,
        in_specs=(spec,) * 4,
        out_specs=(spec,) * 3 + (P(),),
        check_vma=False,
    )
```

```python
import functools
import math

import jax
import jax.numpy as jnp
from jax import lax
from jax.experimental import pallas as pl
from jax.experimental.pallas import tpu as pltpu
from jax.sharding import PartitionSpec as P

MESH = pl.DeviceIdType.MESH
TIME_STEP = 0.05
BITS_PER_WORD = 30
SIDE_X = 4
R = 3
NB = 8
EXT = NB + 2 * R
LANES = 128
REACH = range(-R, R + 1)

FAR = [
    (ez, ex, ey) for ez in (-1, 1) for ex in (0, -1, 1) for ey in (0, -1, 1)
]
NEAR = [(0, ex, ey) for ex in (0, -1, 1) for ey in (0, -1, 1) if (ex, ey) != (0, 0)]
YSLOT = {(ex, ey): i for i, (ex, ey) in enumerate((x, y) for x in (0, -1, 1) for y in (-1, 1))}

CLASSES = {}
for _p in REACH:
    for _r in REACH:
        CLASSES.setdefault(_p * _p + _r * _r, []).append((_p, _r))
CLASSES = sorted(CLASSES.items())


def side(e):
    return 0 if e < 0 else 1


def bond_number(p, q, r):
    flat = (p + R) * 49 + (q + R) * 7 + (r + R)
    return flat if flat < 171 else flat - 1


def weight(p, q, r):
    return 4.0 * math.exp(-(p * p + q * q + r * r) / 9.0)


def kernel(
    sizes,
    disp_hbm,
    vel_hbm,
    body_hbm,
    broken_hbm,
    newd_out,
    newv_out,
    newa_out,
    energy_out,
    disp,
    vel,
    body,
    broken,
    core,
    xpack,
    xrecv,
    ypack,
    yall,
    ynear,
    yfar,
    zrecv,
    zxpack,
    zxrecv,
    yext,
    ext,
    bonds,
    force,
    esum,
    erow,
    eplane,
    ecol,
    load_sem,
    near_send,
    near_recv,
    far_send,
    far_recv,
    esend_sem,
    erecv_sem,
):
    n_gx, n_gy, n_gz = sizes
    gx, gy, gz = lax.axis_index("gx"), lax.axis_index("gy"), lax.axis_index("gz")
    has_low, has_high = gz > 0, gz < n_gz - 1

    def at(ez, ex, ey):
        return (
            lax.rem(gx + ex + n_gx, n_gx),
            lax.rem(gy + ey + n_gy, n_gy),
            gz + ez,
        )

    n_zlo, n_zhi = n_gx // SIDE_X, n_gz // 2
    xs = [lax.rem(gx + d, SIDE_X) for d in range(SIDE_X)]
    ys = [lax.rem(gy + d, n_gy) for d in range(n_gy)]
    cores = [lax.rem(gz + d, 2) for d in range(2)]
    lows = [lax.rem(gx // SIDE_X + d, n_zlo) for d in range(n_zlo)]
    highs = [lax.rem(gz // 2 + d, n_zhi) for d in range(n_zhi)]
    plane = [
        (x, y, c) for x in range(SIDE_X) for y in range(n_gy) for c in range(2)
    ]
    column = [(0, 0, 0, h, l) for h in range(n_zhi) for l in range(n_zlo)]
    stages = (
        [(x, y, c, 0, 0) for x, y, c in plane],
        column,
    )

    def partner(d):
        x, y, c, h, l = d
        return lows[l] * SIDE_X + xs[x], ys[y], highs[h] * 2 + cores[c]

    def place_of(stage, d):
        x, y, c, h, l = d
        if stage == 0:
            return (xs[x] * n_gy + ys[y]) * 2 + cores[c]
        return highs[h] * n_zlo + lows[l]

    def opposite(d):
        sizes = (SIDE_X, n_gy, 2, n_zhi, n_zlo)
        return tuple((n - k) % n for k, n in zip(d, sizes))

    loads = [
        pltpu.make_async_copy(src, dst, load_sem.at[i])
        for i, (src, dst) in enumerate(
            ((disp_hbm, disp), (broken_hbm, broken), (vel_hbm, vel), (body_hbm, body))
        )
    ]
    for load in loads:
        load.start()

    barrier = pltpu.get_barrier_semaphore()

    def greet(device):
        pl.semaphore_signal(barrier, inc=1, device_id=device, device_id_type=MESH)

    for present, low in ((has_low, True), (has_high, False)):

        @pl.when(present)
        def _(low=low):
            for e in FAR:
                if (e[0] < 0) == low:
                    greet(at(*e))

    for e in NEAR:
        greet(at(*e))

    for stage in stages:
        for d in stage[1:]:
            greet(partner(d))

    lane = lax.broadcasted_iota(jnp.int32, (NB, LANES), 1)
    lane2 = lax.broadcasted_iota(jnp.int32, (2 * NB, LANES), 1)
    middle = 0.5 * (NB - 1)
    place = lax.broadcasted_iota(jnp.int32, (NB, LANES), 0).astype(jnp.float32) - middle
    place2 = lax.broadcasted_iota(jnp.int32, (2 * NB, LANES), 0).astype(
        jnp.float32
    ) - (middle + R)

    for present, low in ((has_low, True), (has_high, False)):

        @pl.when(jnp.logical_not(present))
        def _(low=low):
            s = 0 if low else 1
            for step in (0, 1):
                zrecv[step, s] = jnp.zeros(zrecv.shape[2:], jnp.float32)
                zxrecv[step, s] = jnp.zeros(zxrecv.shape[2:], jnp.float32)
                yfar[step, s] = jnp.zeros(yfar.shape[2:], jnp.float32)

    def near_message(step, e, h):
        _, ex, ey = e
        if ey != 0:
            src = yall.at[0, side(ey)] if step == 0 else ypack.at[h, side(ey)]
            dst = ynear.at[step, YSLOT[ex, ey], h]
        elif step == 0:
            src, dst = xpack.at[0, side(ex)], xrecv.at[0, side(ex)]
        else:
            src, dst = xpack.at[1, side(ex), h], xrecv.at[1, side(ex), h]
        return pltpu.make_async_remote_copy(
            src_ref=src,
            dst_ref=dst,
            send_sem=near_send.at[step, NEAR.index(e), h],
            recv_sem=near_recv.at[step, NEAR.index(e), h],
            device_id=at(0, -ex, -ey),
            device_id_type=MESH,
        )

    def far_message(step, e):
        ez, ex, ey = e
        if ey != 0:
            src = yall.at[step, side(ey)]
            dst = yfar.at[step, side(ez), YSLOT[ex, ey]]
        elif ex == 0:
            src = core.at[step, pl.ds(NB - R if ez < 0 else 0, R)]
            dst = zrecv.at[step, side(ez)]
        else:
            src = zxpack.at[step, side(ez), side(ex)]
            dst = zxrecv.at[step, side(ez), side(ex)]
        return pltpu.make_async_remote_copy(
            src_ref=src,
            dst_ref=dst,
            send_sem=far_send.at[step, FAR.index(e)],
            recv_sem=far_recv.at[step, FAR.index(e)],
            device_id=at(-ez, -ex, -ey),
            device_id_type=MESH,
        )

    def for_far(step, present_below, present_above, act):
        for present, below in ((present_below, True), (present_above, False)):

            @pl.when(present)
            def _(below=below):
                for e in FAR:
                    if (e[0] < 0) == below:
                        act(far_message(step, e))

    def send_far(step):
        for_far(step, has_high, has_low, lambda m: m.start())

    def receive_far(step):
        for_far(step, has_low, has_high, lambda m: m.wait_recv())

    def finish_far(step):
        for_far(step, has_high, has_low, lambda m: m.wait_send())

    def pack_pair(step, h):
        ylow, yhigh = yall[step, 0], yall[step, 1]
        for i, z in enumerate((h, NB - 1 - h)):
            for c in range(3):
                g = 3 * (z * 3 + c)
                k = 3 * (i * 3 + c)
                value = core[step, z, c]
                xpack[step, 0, h, k : k + R, :] = core[step, z, c, NB - R : NB, :]
                xpack[step, 1, h, k : k + R, :] = core[step, z, c, 0:R, :]
                mine = (lane >= g) & (lane < g + R)
                ylow = jnp.where(mine, pltpu.roll(value, g + R, 1), ylow)
                yhigh = jnp.where(mine, pltpu.roll(value, g, 1), yhigh)
        yall[step, 0] = ylow
        yall[step, 1] = yhigh
        if step == 1:
            ypack[h, 0] = ylow
            ypack[h, 1] = yhigh

    def pack_far(step):
        for s, base in ((0, NB - R), (1, 0)):
            for i in range(R):
                for c in range(3):
                    k = 3 * (i * 3 + c)
                    zxpack[step, s, 0, k : k + R, :] = core[
                        step, base + i, c, NB - R : NB, :
                    ]
                    zxpack[step, s, 1, k : k + R, :] = core[step, base + i, c, 0:R, :]

    def shift_rows(rows):
        strips = {slot: (yext[slot, 0], yext[slot, 1]) for slot, _, _ in rows}
        here = [[ext[R, row, c] for c in range(3)] for _, row, _ in rows]
        for (slot, row, z), values in zip(rows, here):
            for c in range(3):
                g = 3 * (z * 3 + c)
                left = pltpu.roll(strips[slot][0], LANES - R - g, 1)
                right = pltpu.roll(strips[slot][1], lax.rem(LANES - g, LANES), 1)
                value = values[c]
                if c == 0:
                    left, right, value = left + place2, right + place2, value + place2
                    ext[R, row, c] = value
                for r in range(1, R + 1):
                    after = pltpu.roll(
                        jnp.where(lane2 < r, right, value), LANES - r, 1
                    )
                    before = pltpu.roll(
                        jnp.where(lane2 >= LANES - r, left, value), r, 1
                    )
                    if c == 2:
                        after, before = after + float(r), before - float(r)
                    ext[R + r, row, c] = after
                    ext[R - r, row, c] = before

    def fill_pair(step, h):
        held = 0 if step == 0 else h
        for s, ey in ((0, -1), (1, 1)):
            yext[0, s, R : R + NB, :] = ynear[step, YSLOT[0, ey], held]
            yext[0, s, 0:R, :] = ynear[step, YSLOT[-1, ey], held, NB - R : NB, :]
            yext[0, s, R + NB : EXT, :] = ynear[step, YSLOT[1, ey], held, 0:R, :]
        for i, z in enumerate((h, NB - 1 - h)):
            for c in range(3):
                k = 3 * (i * 3 + c)
                ext[R, z + R, c, R : R + NB, :] = core[step, z, c]
                for s, row in ((0, 0), (1, R + NB)):
                    ext[R, z + R, c, row : row + R, :] = xrecv[
                        step, s, h, k : k + R, :
                    ]
        shift_rows([(0, z + R, z) for z in (h, NB - 1 - h)])

    def fill_far(step):
        for zs, first in ((0, 0), (1, R + NB)):
            for i in range(R):
                for c in range(3):
                    k = 3 * (i * 3 + c)
                    ext[R, first + i, c, R : R + NB, :] = zrecv[step, zs, i, c]
                    for s, row in ((0, 0), (1, R + NB)):
                        ext[R, first + i, c, row : row + R, :] = zxrecv[
                            step, zs, s, k : k + R, :
                        ]
            for s, ey in ((0, -1), (1, 1)):
                yext[zs, s, R : R + NB, :] = yfar[step, zs, YSLOT[0, ey]]
                yext[zs, s, 0:R, :] = yfar[step, zs, YSLOT[-1, ey], NB - R : NB, :]
                yext[zs, s, R + NB : EXT, :] = yfar[step, zs, YSLOT[1, ey], 0:R, :]

        @pl.loop(0, R)
        def _(i):
            shift_rows([(0, i, NB - R + i), (1, R + NB + i, i)])

    def unpack_bonds():
        @pl.loop(0, NB)
        def _(z):
            words = [broken[w, pl.ds(z, NB, stride=NB), :] for w in range(12)]
            depth = gz * NB + z
            for q in REACH:
                inside = (depth + q >= 0) & (depth + q < n_gz * NB)
                scale = jnp.where(inside, 1.0, 0.0)
                for _, members in CLASSES:
                    whole = jnp.full(
                        (NB, LANES), scale * weight(members[0][0], q, members[0][1])
                    )
                    for p, r in members:
                        j = (p + R) * 7 + r + R
                        if (p, q, r) == (0, 0, 0):
                            bonds[z, q + R, j] = jnp.zeros((NB, LANES), jnp.float32)
                            continue
                        k = bond_number(p, q, r)
                        bit = words[k // BITS_PER_WORD] & (1 << (k % BITS_PER_WORD))
                        bonds[z, q + R, j] = jnp.where(bit == 0, whole, 0.0)

    def add_row(step, z, q, task):
        cx, cz, cy = (core[step, z, c] for c in range(3))
        cx = cx + place
        cz = cz - q.astype(jnp.float32)
        row = z + q + R
        fx = fz = fy = energy = None

        def plus(a, b):
            return b if a is None else a + b

        for square, members in CLASSES:
            own = jnp.where(q == 0, 1, 0) if square == 0 else 0
            rest_square = (q * q + square + own).astype(jnp.float32)
            if task != "pull":
                inverse_rest = lax.rsqrt(jnp.full((NB, LANES), rest_square))
            class_energy = None
            cf = [None] * 3
            for p, r in members:
                there = ext.at[r + R, row]
                j = (p + R) * 7 + r + R
                bx = there[0, R + p : R + p + NB, :] - cx
                bz = there[1, R + p : R + p + NB, :] - cz
                by = there[2, R + p : R + p + NB, :] - cy
                pull = bonds[z, q + R, j]
                if task != "pull":
                    length_square = bx * bx + bz * bz + by * by
                    if square == 0:
                        length_square = length_square + own.astype(jnp.float32)
                    gap = inverse_rest - lax.rsqrt(length_square)
                    pull = pull * gap
                if task == "energy":
                    bonds[z, q + R, j] = pull
                    class_energy = plus(class_energy, pull * gap * length_square)
                else:
                    cf = [plus(a, pull * b) for a, b in zip(cf, (bx, bz, by))]
            if task != "energy":
                fx, fz, fy = plus(fx, cf[0]), plus(fz, cf[1]), plus(fy, cf[2])
            if task == "energy":
                rest = jnp.full((NB, LANES), rest_square) * inverse_rest
                energy = plus(energy, class_energy * rest)
        if task == "energy":
            return energy
        force[step, z, 0] += fx
        force[step, z, 1] += fz
        force[step, z, 2] += fy

    def add_pair(step, z, q, task):
        first = add_row(step, z, q, task)
        second = add_row(step, NB - 1 - z, -q, task)
        if task == "energy":
            esum[...] += first + second

    def phase(turn):
        return lax.rem(turn + NB // 2 - 1, NB // 2)

    loads[0].wait()
    for step in (0, 1):
        yall[step] = jnp.zeros(yall.shape[1:], jnp.float32)
        for s in (0, 1):
            for h in range(NB // 2):
                xpack[step, s, h, 16:24, :] = jnp.zeros((NB, LANES), jnp.float32)
            for t in (0, 1):
                zxpack[step, s, t, 24:32, :] = jnp.zeros((NB, LANES), jnp.float32)

    @pl.loop(0, NB // 2)
    def _(h):
        for z in (h, NB - 1 - h):
            for c in range(3):
                core[0, z, c] = disp[c, pl.ds(z, NB, stride=NB), :]
        pack_pair(0, h)

    pack_far(0)
    half = len(FAR) // 2
    greeted = (
        len(NEAR)
        + half * (jnp.where(has_low, 1, 0) + jnp.where(has_high, 1, 0))
        + len(stages[0] + stages[1])
        - 2
    )
    pl.semaphore_wait(barrier, greeted)
    send_far(0)
    for e in NEAR:
        near_message(0, e, 0).start()

    for load in loads[1:]:
        load.wait()
    unpack_bonds()
    esum[...] = jnp.zeros((NB, LANES), jnp.float32)

    @pl.loop(0, NB)
    def _(z):
        for c in range(3):
            value = body[c, pl.ds(z, NB, stride=NB), :]
            force[0, z, c] = value
            force[1, z, c] = value

    for e in NEAR:
        near_message(0, e, 0).wait_recv()

    @pl.loop(0, NB // 2)
    def _(h):
        fill_pair(0, h)

    @pl.loop(0, NB // 2)
    def _(turn):
        h = phase(turn)

        @pl.when(turn == 1)
        def _():
            receive_far(0)
            fill_far(0)

        @pl.loop(0, 2 * R + 1)
        def _(step_q):
            add_pair(0, h, step_q - R, "force")

        for z in (h, NB - 1 - h):
            for c in range(3):
                rows = pl.ds(z, NB, stride=NB)
                moved = (
                    core[0, z, c]
                    + TIME_STEP * vel[c, rows, :]
                    + (0.5 * TIME_STEP * TIME_STEP) * force[0, z, c]
                )
                core[1, z, c] = moved
                newd_out[c, rows, :] = moved
        pack_pair(1, h)
        for e in NEAR:
            near_message(1, e, h).start()

    pack_far(1)
    send_far(1)

    @pl.loop(0, NB // 2)
    def _(turn):
        h = phase(turn)
        for e in NEAR:
            near_message(1, e, h).wait_recv()
        fill_pair(1, h)

        @pl.loop(0, h + R + 1)
        def _(z):
            add_pair(1, z, h - z, "energy")

    receive_far(1)
    fill_far(1)

    @pl.loop(1, R + 1)
    def _(q):
        @pl.loop(NB - q, NB)
        def _(z):
            add_pair(1, z, q, "energy")

    def energy_message(stage, i, sender):
        gathered = (eplane, ecol)[stage]
        return pltpu.make_async_remote_copy(
            src_ref=erow.at[stage],
            dst_ref=gathered.at[place_of(stage, sender)],
            send_sem=esend_sem.at[stage, i],
            recv_sem=erecv_sem.at[stage, i],
            device_id=partner(stages[stage][i]),
            device_id_type=MESH,
        )

    def spread(stage, row):
        me = stages[stage][0]
        erow[stage] = row
        (eplane, ecol)[stage][place_of(stage, me)] = row
        for i in range(1, len(stages[stage])):
            energy_message(stage, i, me).start()

    def gather(stage):
        gathered, count = (eplane, ecol)[stage], len(stages[stage])
        for i in range(1, count):
            energy_message(stage, i, opposite(stages[stage][i])).wait()
        rows = [gathered[m] for m in range(count)]
        while len(rows) > 1:
            rows = [a + b for a, b in zip(rows[::2], rows[1::2])]
        return rows[0]

    spread(0, jnp.sum(esum[...], axis=0, keepdims=True))

    @pl.loop(0, NB // 2)
    def _(h):
        @pl.loop(0, 2 * R + 1)
        def _(t):
            add_pair(1, h, t - R, "pull")

        for z in (h, NB - 1 - h):
            for c in range(3):
                rows = pl.ds(z, NB, stride=NB)
                newa = force[1, z, c]
                newa_out[c, rows, :] = newa
                newv_out[c, rows, :] = vel[c, rows, :] + (0.5 * TIME_STEP) * (
                    force[0, z, c] + newa
                )

    spread(1, gather(0))

    for e in NEAR:
        near_message(0, e, 0).wait_send()

    @pl.loop(0, NB // 2)
    def _(h):
        for e in NEAR:
            near_message(1, e, h).wait_send()

    finish_far(0)
    finish_far(1)
    total = gather(1)
    area = (n_gx * NB) * (n_gy * LANES)
    energy_out[0, 0] = jnp.sum(total) * (0.25 / area)


def hand_out(*refs):
    n = len(refs) // 2
    copies = [
        pltpu.make_async_copy(refs[i], refs[n + i], refs[2 * n].at[i]) for i in range(n)
    ]
    for copy in copies:
        copy.start()
    for copy in copies:
        copy.wait()


def solution(mesh):
    sizes = (mesh.shape["gx"], mesh.shape["gy"], mesh.shape["gz"])
    f32 = jnp.float32
    block = jax.ShapeDtypeStruct((3, NB * NB, LANES), f32)

    def step(displacement, velocity, body_force, broken):
        flat = [
            a.reshape(a.shape[0], NB * NB, LANES)
            for a in (displacement, velocity, body_force, broken)
        ]
        newd, newv, newa, energy = pl.pallas_call(
            functools.partial(kernel, sizes),
            out_shape=(block, block, block, jax.ShapeDtypeStruct((1, 1), f32)),
            in_specs=[pl.BlockSpec(memory_space=pl.ANY)] * 4,
            out_specs=[pl.BlockSpec(memory_space=pltpu.VMEM)] * 3
            + [pl.BlockSpec(memory_space=pltpu.SMEM)],
            scratch_shapes=[
                pltpu.VMEM((3, NB * NB, LANES), f32),
                pltpu.VMEM((3, NB * NB, LANES), f32),
                pltpu.VMEM((3, NB * NB, LANES), f32),
                pltpu.VMEM((12, NB * NB, LANES), jnp.int32),
                pltpu.VMEM((2, NB, 3, NB, LANES), f32),
                pltpu.VMEM((2, 2, NB // 2, 24, LANES), f32),
                pltpu.VMEM((2, 2, NB // 2, 24, LANES), f32),
                pltpu.VMEM((NB // 2, 2, NB, LANES), f32),
                pltpu.VMEM((2, 2, NB, LANES), f32),
                pltpu.VMEM((2, 6, NB // 2, NB, LANES), f32),
                pltpu.VMEM((2, 2, 6, NB, LANES), f32),
                pltpu.VMEM((2, 2, R, 3, NB, LANES), f32),
                pltpu.VMEM((2, 2, 2, 32, LANES), f32),
                pltpu.VMEM((2, 2, 2, 32, LANES), f32),
                pltpu.VMEM((2, 2, 2 * NB, LANES), f32),
                pltpu.VMEM((7, EXT, 3, 2 * NB, LANES), f32),
                pltpu.VMEM((NB, 7, 49, NB, LANES), f32),
                pltpu.VMEM((2, NB, 3, NB, LANES), f32),
                pltpu.VMEM((NB, LANES), f32),
                pltpu.VMEM((2, 1, LANES), f32),
                pltpu.VMEM((32, 1, LANES), f32),
                pltpu.VMEM((8, 1, LANES), f32),
                pltpu.SemaphoreType.DMA((4,)),
                pltpu.SemaphoreType.DMA((2, len(NEAR), NB // 2)),
                pltpu.SemaphoreType.DMA((2, len(NEAR), NB // 2)),
                pltpu.SemaphoreType.DMA((2, len(FAR))),
                pltpu.SemaphoreType.DMA((2, len(FAR))),
                pltpu.SemaphoreType.DMA((2, 32)),
                pltpu.SemaphoreType.DMA((2, 32)),
            ],
            compiler_params=pltpu.CompilerParams(
                collective_id=0,
                has_side_effects=True,
                vmem_limit_bytes=40_000_000,
            ),
        )(*[pltpu.with_memory_space_constraint(a, pltpu.HBM) for a in flat])
        newd, newv, newa = pl.pallas_call(
            hand_out,
            out_shape=(block,) * 3,
            in_specs=[pl.BlockSpec(memory_space=pl.ANY)] * 3,
            out_specs=[pl.BlockSpec(memory_space=pl.ANY)] * 3,
            scratch_shapes=[pltpu.SemaphoreType.DMA((3,))],
            compiler_params=pltpu.CompilerParams(vmem_limit_bytes=40_000_000),
        )(newd, newv, newa)
        shape = displacement.shape
        return (
            newd.reshape(shape),
            newv.reshape(shape),
            newa.reshape(shape),
            energy.reshape(()),
        )

    spec = P(None, "gx", "gz", "gy")
    return jax.shard_map(
        step,
        mesh=mesh,
        in_specs=(spec,) * 4,
        out_specs=(spec,) * 3 + (P(),),
        check_vma=False,
    )
```

```python
import functools
import math

import jax
import jax.numpy as jnp
from jax import lax
from jax.experimental import pallas as pl
from jax.experimental.pallas import tpu as pltpu
from jax.sharding import PartitionSpec as P

MESH = pl.DeviceIdType.MESH
TIME_STEP = 0.05
BITS_PER_WORD = 30
SIDE_X = 4
R = 3
NB = 8
EXT = NB + 2 * R
LANES = 128
REACH = range(-R, R + 1)

FAR = [
    (ez, ex, ey) for ez in (-1, 1) for ex in (0, -1, 1) for ey in (0, -1, 1)
]
NEAR = [(0, ex, ey) for ex in (0, -1, 1) for ey in (0, -1, 1) if (ex, ey) != (0, 0)]
YSLOT = {(ex, ey): i for i, (ex, ey) in enumerate((x, y) for x in (0, -1, 1) for y in (-1, 1))}

CLASSES = {}
for _p in REACH:
    for _r in REACH:
        CLASSES.setdefault(_p * _p + _r * _r, []).append((_p, _r))
CLASSES = sorted(CLASSES.items())


def side(e):
    return 0 if e < 0 else 1


def bond_number(p, q, r):
    flat = (p + R) * 49 + (q + R) * 7 + (r + R)
    return flat if flat < 171 else flat - 1


def weight(p, q, r):
    return 4.0 * math.exp(-(p * p + q * q + r * r) / 9.0)


def kernel(
    sizes,
    disp_hbm,
    vel_hbm,
    body_hbm,
    broken_hbm,
    newd_out,
    newv_out,
    newa_out,
    energy_out,
    disp,
    vel,
    body,
    broken,
    core,
    xpack,
    xrecv,
    ypack,
    yall,
    ynear,
    yfar,
    zrecv,
    zxpack,
    zxrecv,
    yext,
    ext,
    bonds,
    force,
    esum,
    erow,
    eplane,
    ecol,
    load_sem,
    near_send,
    near_recv,
    far_send,
    far_recv,
    early_send,
    early_recv,
    esend_sem,
    erecv_sem,
):
    n_gx, n_gy, n_gz = sizes
    gx, gy, gz = lax.axis_index("gx"), lax.axis_index("gy"), lax.axis_index("gz")
    has_low, has_high = gz > 0, gz < n_gz - 1

    def at(ez, ex, ey):
        return (
            lax.rem(gx + ex + n_gx, n_gx),
            lax.rem(gy + ey + n_gy, n_gy),
            gz + ez,
        )

    n_zlo, n_zhi = n_gx // SIDE_X, n_gz // 2
    xs = [lax.rem(gx + d, SIDE_X) for d in range(SIDE_X)]
    ys = [lax.rem(gy + d, n_gy) for d in range(n_gy)]
    cores = [lax.rem(gz + d, 2) for d in range(2)]
    lows = [lax.rem(gx // SIDE_X + d, n_zlo) for d in range(n_zlo)]
    highs = [lax.rem(gz // 2 + d, n_zhi) for d in range(n_zhi)]
    plane = [
        (x, y, c) for x in range(SIDE_X) for y in range(n_gy) for c in range(2)
    ]
    column = [(0, 0, 0, h, l) for h in range(n_zhi) for l in range(n_zlo)]
    stages = (
        [(x, y, c, 0, 0) for x, y, c in plane],
        column,
    )

    def partner(d):
        x, y, c, h, l = d
        return lows[l] * SIDE_X + xs[x], ys[y], highs[h] * 2 + cores[c]

    def place_of(stage, d):
        x, y, c, h, l = d
        if stage == 0:
            return (xs[x] * n_gy + ys[y]) * 2 + cores[c]
        return highs[h] * n_zlo + lows[l]

    def opposite(d):
        sizes = (SIDE_X, n_gy, 2, n_zhi, n_zlo)
        return tuple((n - k) % n for k, n in zip(d, sizes))

    loads = [
        pltpu.make_async_copy(src, dst, load_sem.at[i])
        for i, (src, dst) in enumerate(
            ((disp_hbm, disp), (broken_hbm, broken), (vel_hbm, vel), (body_hbm, body))
        )
    ]
    for load in loads:
        load.start()

    barrier = pltpu.get_barrier_semaphore()

    def greet(device):
        pl.semaphore_signal(barrier, inc=1, device_id=device, device_id_type=MESH)

    for present, low in ((has_low, True), (has_high, False)):

        @pl.when(present)
        def _(low=low):
            for e in FAR:
                if (e[0] < 0) == low:
                    greet(at(*e))

    for e in NEAR:
        greet(at(*e))

    for stage in stages:
        for d in stage[1:]:
            greet(partner(d))

    lane = lax.broadcasted_iota(jnp.int32, (NB, LANES), 1)
    lane2 = lax.broadcasted_iota(jnp.int32, (2 * NB, LANES), 1)
    middle = 0.5 * (NB - 1)
    place = lax.broadcasted_iota(jnp.int32, (NB, LANES), 0).astype(jnp.float32) - middle
    place2 = lax.broadcasted_iota(jnp.int32, (2 * NB, LANES), 0).astype(
        jnp.float32
    ) - (middle + R)

    for present, low in ((has_low, True), (has_high, False)):

        @pl.when(jnp.logical_not(present))
        def _(low=low):
            s = 0 if low else 1
            for step in (0, 1):
                zrecv[step, s] = jnp.zeros(zrecv.shape[2:], jnp.float32)
                zxrecv[step, s] = jnp.zeros(zxrecv.shape[2:], jnp.float32)
                yfar[step, s] = jnp.zeros(yfar.shape[2:], jnp.float32)

    def near_message(step, e, h):
        _, ex, ey = e
        if ey != 0:
            src = yall.at[0, side(ey)] if step == 0 else ypack.at[h, side(ey)]
            dst = ynear.at[step, YSLOT[ex, ey], h]
        elif step == 0:
            src, dst = xpack.at[0, side(ex)], xrecv.at[0, side(ex)]
        else:
            src, dst = xpack.at[1, side(ex), h], xrecv.at[1, side(ex), h]
        return pltpu.make_async_remote_copy(
            src_ref=src,
            dst_ref=dst,
            send_sem=near_send.at[step, NEAR.index(e), h],
            recv_sem=near_recv.at[step, NEAR.index(e), h],
            device_id=at(0, -ex, -ey),
            device_id_type=MESH,
        )

    def early_message(ez):
        e = (ez, 0, 0)
        return pltpu.make_async_remote_copy(
            src_ref=core.at[1, pl.ds(NB - R + 1 if ez < 0 else 0, R - 1)],
            dst_ref=zrecv.at[1, side(ez), pl.ds(1 if ez < 0 else 0, R - 1)],
            send_sem=early_send.at[side(ez)],
            recv_sem=early_recv.at[side(ez)],
            device_id=at(-ez, 0, 0),
            device_id_type=MESH,
        )

    def far_message(step, e):
        ez, ex, ey = e
        if ey != 0:
            src = yall.at[step, side(ey)]
            dst = yfar.at[step, side(ez), YSLOT[ex, ey]]
        elif ex == 0:
            first, count = (0, R) if step == 0 else (0 if ez < 0 else R - 1, 1)
            src = core.at[step, pl.ds((NB - R if ez < 0 else 0) + first, count)]
            dst = zrecv.at[step, side(ez), pl.ds(first, count)]
        else:
            src = zxpack.at[step, side(ez), side(ex)]
            dst = zxrecv.at[step, side(ez), side(ex)]
        return pltpu.make_async_remote_copy(
            src_ref=src,
            dst_ref=dst,
            send_sem=far_send.at[step, FAR.index(e)],
            recv_sem=far_recv.at[step, FAR.index(e)],
            device_id=at(-ez, -ex, -ey),
            device_id_type=MESH,
        )

    def for_far(step, present_below, present_above, act):
        for present, below in ((present_below, True), (present_above, False)):

            @pl.when(present)
            def _(below=below):
                for e in FAR:
                    if (e[0] < 0) == below:
                        act(far_message(step, e))

    def for_early(present_below, present_above, act):
        for present, ez in ((present_below, -1), (present_above, 1)):

            @pl.when(present)
            def _(ez=ez):
                act(early_message(ez))

    def send_far(step):
        for_far(step, has_high, has_low, lambda m: m.start())

    def receive_far(step):
        for_far(step, has_low, has_high, lambda m: m.wait_recv())
        if step == 1:
            for_early(has_low, has_high, lambda m: m.wait_recv())

    def finish_far(step):
        for_far(step, has_high, has_low, lambda m: m.wait_send())
        if step == 1:
            for_early(has_high, has_low, lambda m: m.wait_send())

    def pack_pair(step, h):
        ylow, yhigh = yall[step, 0], yall[step, 1]
        for i, z in enumerate((h, NB - 1 - h)):
            for c in range(3):
                g = 3 * (z * 3 + c)
                k = 3 * (i * 3 + c)
                value = core[step, z, c]
                xpack[step, 0, h, k : k + R, :] = core[step, z, c, NB - R : NB, :]
                xpack[step, 1, h, k : k + R, :] = core[step, z, c, 0:R, :]
                mine = (lane >= g) & (lane < g + R)
                ylow = jnp.where(mine, pltpu.roll(value, g + R, 1), ylow)
                yhigh = jnp.where(mine, pltpu.roll(value, g, 1), yhigh)
        yall[step, 0] = ylow
        yall[step, 1] = yhigh
        if step == 1:
            ypack[h, 0] = ylow
            ypack[h, 1] = yhigh

    def pack_far(step):
        for s, base in ((0, NB - R), (1, 0)):
            for i in range(R):
                for c in range(3):
                    k = 3 * (i * 3 + c)
                    zxpack[step, s, 0, k : k + R, :] = core[
                        step, base + i, c, NB - R : NB, :
                    ]
                    zxpack[step, s, 1, k : k + R, :] = core[step, base + i, c, 0:R, :]

    def shift_rows(rows):
        strips = {slot: (yext[slot, 0], yext[slot, 1]) for slot, _, _ in rows}
        here = [[ext[R, row, c] for c in range(3)] for _, row, _ in rows]
        for (slot, row, z), values in zip(rows, here):
            for c in range(3):
                g = 3 * (z * 3 + c)
                left = pltpu.roll(strips[slot][0], LANES - R - g, 1)
                right = pltpu.roll(strips[slot][1], lax.rem(LANES - g, LANES), 1)
                value = values[c]
                if c == 0:
                    left, right, value = left + place2, right + place2, value + place2
                    ext[R, row, c] = value
                for r in range(1, R + 1):
                    after = pltpu.roll(
                        jnp.where(lane2 < r, right, value), LANES - r, 1
                    )
                    before = pltpu.roll(
                        jnp.where(lane2 >= LANES - r, left, value), r, 1
                    )
                    if c == 2:
                        after, before = after + float(r), before - float(r)
                    ext[R + r, row, c] = after
                    ext[R - r, row, c] = before

    def fill_pair(step, h):
        held = 0 if step == 0 else h
        for s, ey in ((0, -1), (1, 1)):
            yext[0, s, R : R + NB, :] = ynear[step, YSLOT[0, ey], held]
            yext[0, s, 0:R, :] = ynear[step, YSLOT[-1, ey], held, NB - R : NB, :]
            yext[0, s, R + NB : EXT, :] = ynear[step, YSLOT[1, ey], held, 0:R, :]
        for i, z in enumerate((h, NB - 1 - h)):
            for c in range(3):
                k = 3 * (i * 3 + c)
                ext[R, z + R, c, R : R + NB, :] = core[step, z, c]
                for s, row in ((0, 0), (1, R + NB)):
                    ext[R, z + R, c, row : row + R, :] = xrecv[
                        step, s, h, k : k + R, :
                    ]
        shift_rows([(0, z + R, z) for z in (h, NB - 1 - h)])

    def fill_far(step):
        for zs, first in ((0, 0), (1, R + NB)):
            for i in range(R):
                for c in range(3):
                    k = 3 * (i * 3 + c)
                    ext[R, first + i, c, R : R + NB, :] = zrecv[step, zs, i, c]
                    for s, row in ((0, 0), (1, R + NB)):
                        ext[R, first + i, c, row : row + R, :] = zxrecv[
                            step, zs, s, k : k + R, :
                        ]
            for s, ey in ((0, -1), (1, 1)):
                yext[zs, s, R : R + NB, :] = yfar[step, zs, YSLOT[0, ey]]
                yext[zs, s, 0:R, :] = yfar[step, zs, YSLOT[-1, ey], NB - R : NB, :]
                yext[zs, s, R + NB : EXT, :] = yfar[step, zs, YSLOT[1, ey], 0:R, :]

        @pl.loop(0, R)
        def _(i):
            shift_rows([(0, i, NB - R + i), (1, R + NB + i, i)])

    def unpack_bonds():
        @pl.loop(0, NB)
        def _(z):
            words = [broken[w, pl.ds(z, NB, stride=NB), :] for w in range(12)]
            depth = gz * NB + z
            for q in REACH:
                inside = (depth + q >= 0) & (depth + q < n_gz * NB)
                scale = jnp.where(inside, 1.0, 0.0)
                for _, members in CLASSES:
                    whole = jnp.full(
                        (NB, LANES), scale * weight(members[0][0], q, members[0][1])
                    )
                    for p, r in members:
                        j = (p + R) * 7 + r + R
                        if (p, q, r) == (0, 0, 0):
                            bonds[z, q + R, j] = jnp.zeros((NB, LANES), jnp.float32)
                            continue
                        k = bond_number(p, q, r)
                        bit = words[k // BITS_PER_WORD] & (1 << (k % BITS_PER_WORD))
                        bonds[z, q + R, j] = jnp.where(bit == 0, whole, 0.0)

    def add_row(step, z, q, task):
        cx, cz, cy = (core[step, z, c] for c in range(3))
        cx = cx + place
        cz = cz - q.astype(jnp.float32)
        row = z + q + R
        fx = fz = fy = energy = None

        def plus(a, b):
            return b if a is None else a + b

        for square, members in CLASSES:
            own = jnp.where(q == 0, 1, 0) if square == 0 else 0
            rest_square = (q * q + square + own).astype(jnp.float32)
            if task != "pull":
                inverse_rest = lax.rsqrt(jnp.full((NB, LANES), rest_square))
            class_energy = None
            cf = [None] * 3
            for p, r in members:
                there = ext.at[r + R, row]
                j = (p + R) * 7 + r + R
                bx = there[0, R + p : R + p + NB, :] - cx
                bz = there[1, R + p : R + p + NB, :] - cz
                by = there[2, R + p : R + p + NB, :] - cy
                pull = bonds[z, q + R, j]
                if task != "pull":
                    length_square = bx * bx + bz * bz + by * by
                    if square == 0:
                        length_square = length_square + own.astype(jnp.float32)
                    gap = inverse_rest - lax.rsqrt(length_square)
                    pull = pull * gap
                if task == "energy":
                    bonds[z, q + R, j] = pull
                    class_energy = plus(class_energy, pull * gap * length_square)
                else:
                    cf = [plus(a, pull * b) for a, b in zip(cf, (bx, bz, by))]
            if task != "energy":
                fx, fz, fy = plus(fx, cf[0]), plus(fz, cf[1]), plus(fy, cf[2])
            if task == "energy":
                rest = jnp.full((NB, LANES), rest_square) * inverse_rest
                energy = plus(energy, class_energy * rest)
        if task == "energy":
            return energy
        force[step, z, 0] += fx
        force[step, z, 1] += fz
        force[step, z, 2] += fy

    def add_pair(step, z, q, task):
        first = add_row(step, z, q, task)
        second = add_row(step, NB - 1 - z, -q, task)
        if task == "energy":
            esum[...] += first + second

    def phase(turn):
        return lax.rem(turn + NB // 2 - 1, NB // 2)

    loads[0].wait()
    for step in (0, 1):
        yall[step] = jnp.zeros(yall.shape[1:], jnp.float32)
        for s in (0, 1):
            for h in range(NB // 2):
                xpack[step, s, h, 16:24, :] = jnp.zeros((NB, LANES), jnp.float32)
            for t in (0, 1):
                zxpack[step, s, t, 24:32, :] = jnp.zeros((NB, LANES), jnp.float32)

    @pl.loop(0, NB // 2)
    def _(h):
        for z in (h, NB - 1 - h):
            for c in range(3):
                core[0, z, c] = disp[c, pl.ds(z, NB, stride=NB), :]
        pack_pair(0, h)

    pack_far(0)
    half = len(FAR) // 2
    greeted = (
        len(NEAR)
        + half * (jnp.where(has_low, 1, 0) + jnp.where(has_high, 1, 0))
        + len(stages[0] + stages[1])
        - 2
    )
    pl.semaphore_wait(barrier, greeted)
    send_far(0)
    for e in NEAR:
        near_message(0, e, 0).start()

    for load in loads[1:]:
        load.wait()
    unpack_bonds()
    esum[...] = jnp.zeros((NB, LANES), jnp.float32)

    @pl.loop(0, NB)
    def _(z):
        for c in range(3):
            value = body[c, pl.ds(z, NB, stride=NB), :]
            force[0, z, c] = value
            force[1, z, c] = value

    for e in NEAR:
        near_message(0, e, 0).wait_recv()

    @pl.loop(0, NB // 2)
    def _(h):
        fill_pair(0, h)

    @pl.loop(0, NB // 2)
    def _(turn):
        h = phase(turn)

        @pl.when(turn == 1)
        def _():
            receive_far(0)
            fill_far(0)

        @pl.loop(0, 2 * R + 1)
        def _(step_q):
            add_pair(0, h, step_q - R, "force")

        for z in (h, NB - 1 - h):
            for c in range(3):
                rows = pl.ds(z, NB, stride=NB)
                moved = (
                    core[0, z, c]
                    + TIME_STEP * vel[c, rows, :]
                    + (0.5 * TIME_STEP * TIME_STEP) * force[0, z, c]
                )
                core[1, z, c] = moved
                newd_out[c, rows, :] = moved
        pack_pair(1, h)
        for e in NEAR:
            near_message(1, e, h).start()

        @pl.when(turn == R - 1)
        def _():
            for_early(has_high, has_low, lambda m: m.start())

    pack_far(1)
    send_far(1)

    @pl.loop(0, NB // 2)
    def _(turn):
        h = phase(turn)
        for e in NEAR:
            near_message(1, e, h).wait_recv()
        fill_pair(1, h)

        @pl.loop(0, h + R + 1)
        def _(z):
            add_pair(1, z, h - z, "energy")

    receive_far(1)
    fill_far(1)

    @pl.loop(1, R + 1)
    def _(q):
        @pl.loop(NB - q, NB)
        def _(z):
            add_pair(1, z, q, "energy")

    def energy_message(stage, i, sender):
        gathered = (eplane, ecol)[stage]
        return pltpu.make_async_remote_copy(
            src_ref=erow.at[stage],
            dst_ref=gathered.at[place_of(stage, sender)],
            send_sem=esend_sem.at[stage, i],
            recv_sem=erecv_sem.at[stage, i],
            device_id=partner(stages[stage][i]),
            device_id_type=MESH,
        )

    def spread(stage, row):
        me = stages[stage][0]
        erow[stage] = row
        (eplane, ecol)[stage][place_of(stage, me)] = row
        for i in range(1, len(stages[stage])):
            energy_message(stage, i, me).start()

    def gather(stage):
        gathered, count = (eplane, ecol)[stage], len(stages[stage])
        for i in range(1, count):
            energy_message(stage, i, opposite(stages[stage][i])).wait()
        rows = [gathered[m] for m in range(count)]
        while len(rows) > 1:
            rows = [a + b for a, b in zip(rows[::2], rows[1::2])]
        return rows[0]

    spread(0, jnp.sum(esum[...], axis=0, keepdims=True))

    @pl.loop(0, NB // 2)
    def _(h):
        @pl.loop(0, 2 * R + 1)
        def _(t):
            add_pair(1, h, t - R, "pull")

        for z in (h, NB - 1 - h):
            for c in range(3):
                rows = pl.ds(z, NB, stride=NB)
                newa = force[1, z, c]
                newa_out[c, rows, :] = newa
                newv_out[c, rows, :] = vel[c, rows, :] + (0.5 * TIME_STEP) * (
                    force[0, z, c] + newa
                )

    spread(1, gather(0))

    for e in NEAR:
        near_message(0, e, 0).wait_send()

    @pl.loop(0, NB // 2)
    def _(h):
        for e in NEAR:
            near_message(1, e, h).wait_send()

    finish_far(0)
    finish_far(1)
    total = gather(1)
    area = (n_gx * NB) * (n_gy * LANES)
    energy_out[0, 0] = jnp.sum(total) * (0.25 / area)


def hand_out(*refs):
    n = len(refs) // 2
    copies = [
        pltpu.make_async_copy(refs[i], refs[n + i], refs[2 * n].at[i]) for i in range(n)
    ]
    for copy in copies:
        copy.start()
    for copy in copies:
        copy.wait()


def solution(mesh):
    sizes = (mesh.shape["gx"], mesh.shape["gy"], mesh.shape["gz"])
    f32 = jnp.float32
    block = jax.ShapeDtypeStruct((3, NB * NB, LANES), f32)

    def step(displacement, velocity, body_force, broken):
        flat = [
            a.reshape(a.shape[0], NB * NB, LANES)
            for a in (displacement, velocity, body_force, broken)
        ]
        newd, newv, newa, energy = pl.pallas_call(
            functools.partial(kernel, sizes),
            out_shape=(block, block, block, jax.ShapeDtypeStruct((1, 1), f32)),
            in_specs=[pl.BlockSpec(memory_space=pl.ANY)] * 4,
            out_specs=[pl.BlockSpec(memory_space=pltpu.VMEM)] * 3
            + [pl.BlockSpec(memory_space=pltpu.SMEM)],
            scratch_shapes=[
                pltpu.VMEM((3, NB * NB, LANES), f32),
                pltpu.VMEM((3, NB * NB, LANES), f32),
                pltpu.VMEM((3, NB * NB, LANES), f32),
                pltpu.VMEM((12, NB * NB, LANES), jnp.int32),
                pltpu.VMEM((2, NB, 3, NB, LANES), f32),
                pltpu.VMEM((2, 2, NB // 2, 24, LANES), f32),
                pltpu.VMEM((2, 2, NB // 2, 24, LANES), f32),
                pltpu.VMEM((NB // 2, 2, NB, LANES), f32),
                pltpu.VMEM((2, 2, NB, LANES), f32),
                pltpu.VMEM((2, 6, NB // 2, NB, LANES), f32),
                pltpu.VMEM((2, 2, 6, NB, LANES), f32),
                pltpu.VMEM((2, 2, R, 3, NB, LANES), f32),
                pltpu.VMEM((2, 2, 2, 32, LANES), f32),
                pltpu.VMEM((2, 2, 2, 32, LANES), f32),
                pltpu.VMEM((2, 2, 2 * NB, LANES), f32),
                pltpu.VMEM((7, EXT, 3, 2 * NB, LANES), f32),
                pltpu.VMEM((NB, 7, 49, NB, LANES), f32),
                pltpu.VMEM((2, NB, 3, NB, LANES), f32),
                pltpu.VMEM((NB, LANES), f32),
                pltpu.VMEM((2, 1, LANES), f32),
                pltpu.VMEM((32, 1, LANES), f32),
                pltpu.VMEM((8, 1, LANES), f32),
                pltpu.SemaphoreType.DMA((4,)),
                pltpu.SemaphoreType.DMA((2, len(NEAR), NB // 2)),
                pltpu.SemaphoreType.DMA((2, len(NEAR), NB // 2)),
                pltpu.SemaphoreType.DMA((2, len(FAR))),
                pltpu.SemaphoreType.DMA((2, len(FAR))),
                pltpu.SemaphoreType.DMA((2,)),
                pltpu.SemaphoreType.DMA((2,)),
                pltpu.SemaphoreType.DMA((2, 32)),
                pltpu.SemaphoreType.DMA((2, 32)),
            ],
            compiler_params=pltpu.CompilerParams(
                collective_id=0,
                has_side_effects=True,
                vmem_limit_bytes=40_000_000,
            ),
        )(*[pltpu.with_memory_space_constraint(a, pltpu.HBM) for a in flat])
        newd, newv, newa = pl.pallas_call(
            hand_out,
            out_shape=(block,) * 3,
            in_specs=[pl.BlockSpec(memory_space=pl.ANY)] * 3,
            out_specs=[pl.BlockSpec(memory_space=pl.ANY)] * 3,
            scratch_shapes=[pltpu.SemaphoreType.DMA((3,))],
            compiler_params=pltpu.CompilerParams(vmem_limit_bytes=40_000_000),
        )(newd, newv, newa)
        shape = displacement.shape
        return (
            newd.reshape(shape),
            newv.reshape(shape),
            newa.reshape(shape),
            energy.reshape(()),
        )

    spec = P(None, "gx", "gz", "gy")
    return jax.shard_map(
        step,
        mesh=mesh,
        in_specs=(spec,) * 4,
        out_specs=(spec,) * 3 + (P(),),
        check_vma=False,
    )
```
